512 devices in a mesh: parts: 2 (over y), row: 32 (over z), col: 4 (over x), sub: 2 (over core).
Axes of the slice: x: 4, y: 2, z: 32, core: 2. Of those that a mesh axis runs over, the one named last changes fastest.
The devices are a block of a 4x16x32 slice.
Arguments:
- pair: float32 [768, 384, 128], P(('parts', 'row'), ('col', 'sub')), parts along dimension 0, may hold values from -250 to 250, as said below
- residue_mask: int32 [768], P('parts'), parts along dimension 0, may hold values from 0 to 1, as said below
- tri_norm_gain: float32 [128], replicated, may hold values from 0.25 to 1.75
- tri_in_weight: bfloat16 [128, 4, 128], replicated, may hold values from -0.5 to 0.5
- tri_gate_weight: bfloat16 [128, 128], replicated, may hold values from -0.5 to 0.5
- tri_out_norm_gain: float32 [128], replicated, may hold values from 0.25 to 1.75
- tri_out_weight: bfloat16 [128, 128], replicated, may hold values from -0.5 to 0.5
- att_norm_gain: float32 [128], replicated, may hold values from 0.25 to 1.75
- att_proj_weight: bfloat16 [128, 4, 128], replicated, may hold values from -0.5 to 0.5
- att_bias_weight: bfloat16 [128, 4], replicated, may hold values from -15 to 15
- att_out_weight: bfloat16 [128, 128], replicated, may hold values from -0.5 to 0.5
Outputs:
- pair_out: float32 [768, 384, 128], P(('parts', 'row'), ('col', 'sub')), parts along dimension 0
The draws below stay inside these ranges and needn't reach their ends.
There are 2 independent parts, one for each index of `parts`. The reference program is written for one: setup_inputs(seed, part) draws one part's arguments, and reference() takes and returns one part's arrays. A program takes and returns all parts, laid end to end along the dimension named above; an argument that names none is the same for every part. Nothing has to cross between parts.
Inputs may be any that keep to these rules, and one draw needn't show every extreme that they name: The pair entries are finite. `residue_mask`: 0 on every residue at or above a length of at least 192 and less than 384; below it 1, except some unresolved residues that are 0; residue 0 is always 1.
All inputs are finite; a program needn't handle non-finite values.
Results may differ from the reference program's by a relative error of at most 0.0032.
Values may be sent and summed in bfloat16 or wider, within the bound.
A program may use at most 64 MiB of HBM per device.

```python
import math
import jax
import jax.numpy as jnp
from jax import lax

PAIR_CH = 128
TRI_HID = 128
HEADS = 4
HEAD_DIM = 32
RESIDUES = 384


def draw_pair(key, part):
    base_draw = jnp.clip(jax.random.normal(key, (RESIDUES, RESIDUES, PAIR_CH), jnp.float32), -6.0, 6.0)
    return base_draw


def draw_residue_mask(key, part):
    length = jax.random.randint(jax.random.fold_in(key, 7), (), RESIDUES // 2, RESIDUES)
    kept = jax.random.randint(jax.random.fold_in(key, 8), (RESIDUES,), 0, 8) != 0
    positions = jnp.arange(RESIDUES)
    live = (positions < length) & (kept | (positions == 0))
    return live.astype(jnp.int32)


def draw_att_bias_weight(key, part):
    base_draw = jnp.clip(jax.random.normal(key, (PAIR_CH, HEADS), jnp.float32), -4.0, 4.0)
    spread = 2.0
    return jnp.clip(base_draw * (spread / math.sqrt(PAIR_CH)), -15.0, 15.0).astype(jnp.bfloat16)


def gaussian(own_key, extent, scale, most, dtype=jnp.bfloat16):
    entries = jax.random.normal(own_key, extent, jnp.float32) * scale
    return jnp.minimum(jnp.maximum(entries, -most), most).astype(dtype)


def setup_inputs(seed: int = 0, part: int = 0) -> dict:
    streams_of = jax.random.split(jax.random.key(seed), 12)
    part_keys = jax.random.split(jax.random.fold_in(streams_of[11], part), 12)
    return {
        "pair": draw_pair(jax.random.fold_in(jax.random.fold_in(streams_of[11], part), 71), part),
        "residue_mask": draw_residue_mask(jax.random.fold_in(jax.random.fold_in(streams_of[11], part), 71), part),
        "tri_norm_gain": jnp.clip(1.0 + 0.15 * jax.random.normal(streams_of[2], (PAIR_CH,), jnp.float32), 0.25, 1.75),
        "tri_in_weight": gaussian(streams_of[3], (PAIR_CH, 4, TRI_HID), PAIR_CH ** -0.5, 0.5),
        "tri_gate_weight": gaussian(streams_of[4], (PAIR_CH, PAIR_CH), PAIR_CH ** -0.5, 0.5),
        "tri_out_norm_gain": jnp.clip(1.0 + 0.15 * jax.random.normal(streams_of[5], (TRI_HID,), jnp.float32), 0.25, 1.75),
        "tri_out_weight": gaussian(streams_of[6], (TRI_HID, PAIR_CH), TRI_HID ** -0.5, 0.5),
        "att_norm_gain": jnp.clip(1.0 + 0.15 * jax.random.normal(streams_of[7], (PAIR_CH,), jnp.float32), 0.25, 1.75),
        "att_proj_weight": gaussian(streams_of[8], (PAIR_CH, 4, HEADS * HEAD_DIM), PAIR_CH ** -0.5, 0.5),
        "att_bias_weight": draw_att_bias_weight(jax.random.fold_in(streams_of[11], 71), part),
        "att_out_weight": gaussian(streams_of[10], (HEADS * HEAD_DIM, PAIR_CH), (HEADS * HEAD_DIM) ** -0.5, 0.5),
    }


epsilon = 1e-05
mask_penalty = 1000000000.0

def norm_last(values_in, gain):
    center = lax.optimization_barrier(jnp.mean(values_in, axis=-1, keepdims=True))
    centered = values_in - center
    variance = lax.optimization_barrier(jnp.mean(centered * centered, axis=-1, keepdims=True))
    return centered * lax.rsqrt(variance + epsilon) * gain

def project(normed, weight):
    flat_rows = normed.reshape(-1, normed.shape[-1])
    product = jnp.dot(flat_rows, weight, preferred_element_type=jnp.float32)
    return product.reshape(normed.shape[:-1] + (weight.shape[1],))

def reference(pair, residue_mask, tri_norm_gain, tri_in_weight, tri_gate_weight, tri_out_norm_gain, tri_out_weight, att_norm_gain, att_proj_weight, att_bias_weight, att_out_weight):
    residue_live = residue_mask.astype(jnp.float32)
    pair_live = (residue_live[:, None] * residue_live[None, :])[:, :, None]
    tri_normed = norm_last(pair, tri_norm_gain).astype(jnp.bfloat16)
    left_factor = (jax.nn.sigmoid(project(tri_normed, tri_in_weight[:, 0])) * project(tri_normed, tri_in_weight[:, 1]) * pair_live).astype(jnp.bfloat16)
    right_factor = (jax.nn.sigmoid(project(tri_normed, tri_in_weight[:, 2])) * project(tri_normed, tri_in_weight[:, 3]) * pair_live).astype(jnp.bfloat16)
    tri_sum = jnp.einsum('ikh,jkh->ijh', left_factor.astype(jnp.float32), right_factor.astype(jnp.float32))
    hidden_normed = norm_last(tri_sum, tri_out_norm_gain).astype(jnp.bfloat16)
    tri_gate = jax.nn.sigmoid(project(tri_normed, tri_gate_weight))
    pair_mid = pair + tri_gate * project(hidden_normed, tri_out_weight)
    att_normed = norm_last(pair_mid, att_norm_gain).astype(jnp.bfloat16)
    head_shape = (RESIDUES, RESIDUES, HEADS, HEAD_DIM)
    queries = (project(att_normed, att_proj_weight[:, 0]) * HEAD_DIM ** (-0.5)).astype(jnp.bfloat16).reshape(head_shape)
    key_rows = project(att_normed, att_proj_weight[:, 1]).astype(jnp.bfloat16).reshape(head_shape)
    value_rows = project(att_normed, att_proj_weight[:, 2]).astype(jnp.bfloat16).reshape(head_shape)
    att_gate = jax.nn.sigmoid(project(att_normed, att_proj_weight[:, 3]))
    pair_bias = project(att_normed, att_bias_weight).astype(jnp.bfloat16)
    mask_row = (residue_live - 1.0) * mask_penalty
    head_bias = jnp.transpose(pair_bias.astype(jnp.float32), (2, 0, 1)) + mask_row[None, None, :]

    def one_row(row_item):
        query_row, key_row, value_row = row_item
        scores = jnp.einsum('jhd,khd->hjk', query_row.astype(jnp.float32), key_row.astype(jnp.float32)) + head_bias
        row_max = lax.optimization_barrier(jnp.max(scores, axis=-1, keepdims=True))
        raised = jnp.exp(scores - row_max)
        weights = (raised / lax.optimization_barrier(jnp.sum(raised, axis=-1, keepdims=True))).astype(jnp.bfloat16)
        return jnp.einsum('hjk,khd->jhd', weights.astype(jnp.float32), value_row.astype(jnp.float32))
    attended = lax.map(one_row, (queries, key_rows, value_rows))
    gated = (attended.reshape(RESIDUES, RESIDUES, HEADS * HEAD_DIM) * att_gate).astype(jnp.bfloat16)
    return pair_mid + project(gated, att_out_weight)
```

```python
import functools

import jax
import jax.numpy as jnp
from jax import lax
from jax.experimental import pallas as pl
from jax.experimental.pallas import tpu as pltpu
from jax.sharding import PartitionSpec as P

MESH = pl.DeviceIdType.MESH
EPSILON = 1e-05
MASK_PENALTY = 1000000000.0
F32 = jnp.float32
BF16 = jnp.bfloat16
CHUNKS = 4


def norm_last(values_in, gain):
    center = jnp.mean(values_in, axis=-1, keepdims=True)
    centered = values_in - center
    variance = jnp.mean(centered * centered, axis=-1, keepdims=True)
    return centered * lax.rsqrt(variance + EPSILON) * gain


def dot(a, b):
    return lax.dot_general(a, b, (((1,), (0,)), ((), ())), preferred_element_type=F32)


def dot_nt(a, b):
    return lax.dot_general(a, b, (((1,), (1,)), ((), ())), preferred_element_type=F32)


def one_hot(rows, cols, match):
    r = lax.broadcasted_iota(jnp.int32, (rows, cols), 0)
    c = lax.broadcasted_iota(jnp.int32, (rows, cols), 1)
    return jnp.where(match(r, c), 1.0, 0.0).astype(BF16)


def kernel(
    planes,
    groups,
    subs,
    heads,
    pair_ref,
    live_row_ref,
    live_col_ref,
    mask_ref,
    gain1_ref,
    w_in_ref,
    w_gate_ref,
    gain2_ref,
    w_tri_ref,
    gain3_ref,
    w_att_ref,
    w_bias_ref,
    w_out_ref,
    out_ref,
    right_buf,
    left_buf,
    normed_buf,
    part_buf,
    sum_buf,
    tmp_buf,
    tri_buf,
    att_buf,
    key_buf,
    value_buf,
    query_buf,
    gate_buf,
    score_buf,
    mid_buf,
    bias_rows,
    bias_z,
    bias_x,
    bias_buf,
    gated_buf,
    ring_send,
    ring_recv,
    part_send,
    part_recv,
    att_send,
    att_recv,
    bz_send,
    bz_recv,
    bx_send,
    bx_recv,
):
    rows, cols, chan = pair_ref.shape
    flat = rows * cols
    per_owner = planes // groups
    residues = groups * cols
    z = lax.axis_index("row")
    g = lax.axis_index(("col", "sub"))
    z_up = lax.rem(z + 1, planes)
    z_down = lax.rem(z + planes - 1, planes)

    def in_plane(c):
        return {"col": c // subs, "sub": lax.rem(c, subs)}

    barrier = pltpu.get_barrier_semaphore()
    for other in (z_up, z_down):
        pl.semaphore_signal(barrier, inc=1, device_id={"row": other}, device_id_type=MESH)
    for d in range(1, groups):
        pl.semaphore_signal(
            barrier, inc=1, device_id=in_plane(lax.rem(g + d, groups)), device_id_type=MESH
        )

    pair = pair_ref[...].reshape(flat, chan)
    normed = norm_last(pair, gain1_ref[...]).astype(BF16)
    normed_buf[...] = normed
    live_rows = live_row_ref[z]
    live_cols = live_col_ref[g]
    live = jnp.concatenate([live_rows[i : i + 1] * live_cols for i in range(rows)], axis=0)

    def factor(p):
        gate = dot(normed, w_in_ref[:, p * chan : (p + 1) * chan])
        value = dot(normed, w_in_ref[:, (p + 1) * chan : (p + 2) * chan])
        return (jax.nn.sigmoid(gate) * value * live).astype(BF16)

    right_buf[z] = factor(2).reshape(rows, cols, chan)
    pl.semaphore_wait(barrier, groups + 1)

    chunk_rows = rows // CHUNKS
    half = planes // 2
    last = half - 1

    def ring_copy(way, step, chunk):
        origin = lax.rem(z + planes - step, planes) if way == 0 else lax.rem(z + step, planes)
        block = right_buf.at[origin, pl.ds(chunk * chunk_rows, chunk_rows)]
        return pltpu.make_async_remote_copy(
            src_ref=block,
            dst_ref=block,
            send_sem=ring_send.at[way, step, chunk],
            recv_sem=ring_recv.at[way, step, chunk],
            device_id={"row": z_up if way == 0 else z_down},
            device_id_type=MESH,
        )

    def ring_arrival(way, step, chunk):
        origin = (
            lax.rem(z + 2 * planes - 1 - step, planes) if way == 0 else lax.rem(z + 1 + step, planes)
        )
        block = right_buf.at[origin, pl.ds(chunk * chunk_rows, chunk_rows)]
        pltpu.make_async_remote_copy(
            src_ref=block,
            dst_ref=block,
            send_sem=ring_send.at[way, step, chunk],
            recv_sem=ring_recv.at[way, step, chunk],
            device_id={"row": z_up if way == 0 else z_down},
            device_id_type=MESH,
        ).wait_recv()
        return origin

    halves = (range(CHUNKS // 2), range(CHUNKS // 2, CHUNKS))
    for chunk in range(CHUNKS):
        for way in range(2):
            ring_copy(way, 0, chunk).start()

    left_buf[...] = factor(0).astype(F32).reshape(rows, cols, chan)

    def products(origin, chunk):
        for j in range(chunk * chunk_rows, (chunk + 1) * chunk_rows):
            right = right_buf[origin, j].astype(F32)
            part_buf[origin, j * rows : (j + 1) * rows, :] = jnp.sum(
                left_buf[...] * right[None], axis=1
            )

    def part_copy(origin):
        owner = origin // per_owner
        return pltpu.make_async_remote_copy(
            src_ref=part_buf.at[origin],
            dst_ref=sum_buf.at[g, lax.rem(origin, per_owner)],
            send_sem=part_send.at[origin],
            recv_sem=part_recv.at[g, lax.rem(origin, per_owner)],
            device_id=in_plane(owner),
            device_id_type=MESH,
        )

    def to_owner(origin):
        @pl.when(origin // per_owner != g)
        def _():
            part_copy(origin).start()

    for chunk in range(CHUNKS):
        products(z, chunk)
    to_owner(z)

    def ring_step(step, carry):
        up = down = None
        for chunk in range(CHUNKS):
            for way in range(2):
                origin = ring_arrival(way, step, chunk)
                if chunk in halves[way]:
                    ring_copy(way, step + 1, chunk).start()
                else:

                    @pl.when(step + 1 < last)
                    def _():
                        ring_copy(way, step + 1, chunk).start()

                if way == 0:
                    up = origin
                else:
                    down = origin
            products(up, chunk)
            products(down, chunk)
        to_owner(up)
        to_owner(down)
        return carry

    lax.fori_loop(0, last, ring_step, 0)
    far = lax.rem(z + half, planes)
    for pair_of in zip(*halves):
        for way, chunk in enumerate(pair_of):
            ring_arrival(way, last, chunk)
            products(far, chunk)
    to_owner(far)

    tri_gate = jax.nn.sigmoid(dot(normed_buf[...], w_gate_ref[...]))

    block = rows * rows
    for p in range(per_owner):
        total = part_buf[g * per_owner + p]
        for d in range(1, groups):
            c = lax.rem(g + d, groups)
            pltpu.make_async_remote_copy(
                src_ref=part_buf.at[p],
                dst_ref=sum_buf.at[c, p],
                send_sem=part_send.at[p],
                recv_sem=part_recv.at[c, p],
                device_id=in_plane(c),
                device_id_type=MESH,
            ).wait_recv()
            total = total + sum_buf[c, p]
        tmp_buf[p * block : (p + 1) * block, :] = total
    for i in range(rows):
        tri_buf[i * cols : (i + 1) * cols, :] = tmp_buf[pl.ds(i, cols, stride=rows), :]

    hidden = norm_last(tri_buf[...], gain2_ref[...]).astype(BF16)
    pair_mid = pair_ref[...].reshape(flat, chan) + tri_gate * dot(hidden, w_tri_ref[...])
    mid_buf[...] = pair_mid
    att = norm_last(pair_mid, gain3_ref[...]).astype(BF16)
    att_buf[g] = att.reshape(rows, cols, chan)

    for j in range(rows):
        bias_rows[j * 8 : (j + 1) * 8, :] = dot_nt(
            w_bias_ref[...], att[j * cols : (j + 1) * cols, :]
        )
    packed_rows = bias_z.shape[1]
    half_rows = rows // 2
    stacked = bias_rows[...].astype(BF16)
    message = jnp.zeros((packed_rows, chan), F32)
    for q in range(2):
        pick = one_hot(
            packed_rows,
            rows * 8,
            lambda r, c: c == (q * half_rows + lax.rem(r, half_rows)) * 8 + r // half_rows,
        )
        spread = one_hot(cols, chan, lambda r, c: c == r + q * cols)
        message = message + dot(dot(pick, stacked).astype(BF16), spread)
    bias_z[z] = message.astype(BF16)

    def bz_copy(source, target):
        return pltpu.make_async_remote_copy(
            src_ref=bias_z.at[source],
            dst_ref=bias_z.at[source],
            send_sem=bz_send.at[target],
            recv_sem=bz_recv.at[source],
            device_id={"row": target},
            device_id_type=MESH,
        )

    def send_bias(k, carry):
        bz_copy(z, lax.rem(z + half + k, planes)).start()
        bz_copy(z, lax.rem(z + half - k, planes)).start()
        return carry

    bz_copy(z, lax.rem(z + half, planes)).start()
    lax.fori_loop(1, half, send_bias, 0)

    def att_copy(source, target):
        return pltpu.make_async_remote_copy(
            src_ref=att_buf.at[source],
            dst_ref=att_buf.at[source],
            send_sem=att_send.at[target],
            recv_sem=att_recv.at[source],
            device_id=in_plane(target),
            device_id_type=MESH,
        )

    for d in range(1, groups):
        att_copy(g, lax.rem(g + d, groups)).start()

    scale = (chan // heads) ** (-0.5)
    query_buf[...] = (dot(att, w_att_ref[:, :chan]) * scale).astype(BF16)
    gate_buf[...] = jax.nn.sigmoid(dot(att, w_att_ref[:, 3 * chan :]))

    for d in range(groups):
        c = lax.rem(g + d, groups)
        if d:
            att_copy(c, g).wait_recv()
        here = pl.ds(pl.multiple_of(c * cols, cols), cols)
        both = dot(att_buf[c].reshape(flat, chan), w_att_ref[:, chan : 3 * chan]).astype(BF16)
        key_buf[:, here, :] = both[:, :chan].reshape(rows, cols, chan)
        value_buf[:, here, :] = both[:, chan:].reshape(rows, cols, chan)

    lane_head = lax.broadcasted_iota(jnp.int32, (cols, chan), 1) // (chan // heads)

    def raw_scores(i, carry):
        query = query_buf[pl.ds(pl.multiple_of(i * cols, cols), cols), :]
        stack = jnp.concatenate(
            [jnp.where(lane_head == h, query, jnp.zeros_like(query)) for h in range(heads)], axis=0
        )
        score_buf[i] = dot_nt(stack, key_buf[i])
        return carry

    lax.fori_loop(0, rows, raw_scores, 0)

    def bx_copy(source, target):
        return pltpu.make_async_remote_copy(
            src_ref=bias_z.at[pl.ds(target * per_owner, per_owner)],
            dst_ref=bias_x.at[source],
            send_sem=bx_send.at[target],
            recv_sem=bx_recv.at[source],
            device_id=in_plane(target),
            device_id_type=MESH,
        )

    for d in range(groups):
        c = lax.rem(g + d, groups)
        for p in range(per_owner):
            source = c * per_owner + p

            @pl.when(source != z)
            def _():
                bz_copy(source, z).wait_recv()

        if d:
            bx_copy(g, c).start()

    sums = [jnp.zeros((per_owner * packed_rows, residues), F32) for _ in range(2)]
    for d in range(groups):
        c = lax.rem(g + d, groups)
        if d:
            bx_copy(c, g).wait_recv()
            piece = bias_x[c]
        else:
            piece = bias_z[pl.ds(g * per_owner, per_owner)]
        piece = piece.reshape(per_owner * packed_rows, chan)
        for q in range(2):
            spread = one_hot(
                chan, residues, lambda r, k: (k - c * cols == r - q * cols) & (r >= q * cols) & (r < (q + 1) * cols)
            )
            sums[q] = sums[q] + dot(piece, spread)
    bias = jnp.zeros((heads * cols, residues), F32)
    for q in range(2):
        def match(r, c):
            h, j = r // cols, lax.rem(r, cols)
            p, j = j // rows, lax.rem(j, rows)
            return (j // half_rows == q) & (
                c == p * packed_rows + h * half_rows + lax.rem(j, half_rows)
            )

        bias = bias + dot(
            one_hot(heads * cols, per_owner * packed_rows, match), sums[q].astype(BF16)
        )
    bias_buf[...] = bias + mask_ref[...]

    def attend(i, carry):
        scores = score_buf[i] + bias_buf[...]
        raised = jnp.exp(scores - jnp.max(scores, axis=-1, keepdims=True))
        weights = (raised * (1.0 / jnp.sum(raised, axis=-1, keepdims=True))).astype(BF16)
        mixed = dot(weights, value_buf[i])
        attended = jnp.zeros((cols, chan), F32)
        for h in range(heads):
            attended = jnp.where(lane_head == h, mixed[h * cols : (h + 1) * cols, :], attended)
        here = pl.ds(pl.multiple_of(i * cols, cols), cols)
        gated_buf[here, :] = (attended * gate_buf[here, :]).astype(BF16)
        return carry

    lax.fori_loop(0, rows, attend, 0)
    out_ref[...] = (mid_buf[...] + dot(gated_buf[...], w_out_ref[...])).reshape(rows, cols, chan)

    def ring_sent(step, carry):
        for way in range(2):
            for chunk in range(CHUNKS):
                ring_copy(way, step, chunk).wait_send()
        return carry

    lax.fori_loop(0, last, ring_sent, 0)
    for way in range(2):
        for chunk in halves[way]:
            ring_copy(way, last, chunk).wait_send()

    def parts_sent(origin, carry):
        @pl.when(origin // per_owner != g)
        def _():
            part_copy(origin).wait_send()

        @pl.when(origin != z)
        def _():
            bz_copy(z, origin).wait_send()

        return carry

    lax.fori_loop(0, planes, parts_sent, 0)
    for d in range(1, groups):
        c = lax.rem(g + d, groups)
        att_copy(g, c).wait_send()
        bx_copy(g, c).wait_send()


def solution(mesh):
    planes = mesh.shape["row"]
    subs = mesh.shape["sub"]
    groups = mesh.shape["col"] * subs

    def body(
        pair,
        residue_mask,
        tri_norm_gain,
        tri_in_weight,
        tri_gate_weight,
        tri_out_norm_gain,
        tri_out_weight,
        att_norm_gain,
        att_proj_weight,
        att_bias_weight,
        att_out_weight,
    ):
        rows, cols, chan = pair.shape
        heads = att_bias_weight.shape[1]
        residues = residue_mask.shape[0]
        live = residue_mask.astype(F32)
        live_row = jnp.broadcast_to(live.reshape(planes, rows, 1), (planes, rows, chan))
        live_col = jnp.broadcast_to(live.reshape(groups, cols, 1), (groups, cols, chan))
        mask_row = ((live - 1.0) * MASK_PENALTY)[None, :]
        w_bias = jnp.concatenate(
            [att_bias_weight.T, jnp.zeros((8 - heads, chan), att_bias_weight.dtype)], axis=0
        )
        flat = rows * cols
        per_owner = planes // groups
        packed = heads * rows // 2
        vmem = pl.BlockSpec(memory_space=pltpu.VMEM)
        dma = pltpu.SemaphoreType.DMA
        operands = (
            pair,
            live_row,
            live_col,
            mask_row,
            tri_norm_gain[None, :],
            tri_in_weight.reshape(chan, -1),
            tri_gate_weight,
            tri_out_norm_gain[None, :],
            tri_out_weight,
            att_norm_gain[None, :],
            att_proj_weight.reshape(chan, -1),
            w_bias,
            att_out_weight,
        )
        return pl.pallas_call(
            functools.partial(kernel, planes, groups, subs, heads),
            out_shape=jax.ShapeDtypeStruct(pair.shape, F32),
            in_specs=[vmem] * len(operands),
            out_specs=vmem,
            scratch_shapes=[
                pltpu.VMEM((planes, rows, cols, chan), BF16),
                pltpu.VMEM((rows, cols, chan), F32),
                pltpu.VMEM((flat, chan), BF16),
                pltpu.VMEM((planes, rows * rows, chan), F32),
                pltpu.VMEM((groups, per_owner, rows * rows, chan), F32),
                pltpu.VMEM((flat, chan), F32),
                pltpu.VMEM((flat, chan), F32),
                pltpu.VMEM((groups, rows, cols, chan), BF16),
                pltpu.VMEM((rows, residues, chan), BF16),
                pltpu.VMEM((rows, residues, chan), BF16),
                pltpu.VMEM((flat, chan), BF16),
                pltpu.VMEM((flat, chan), F32),
                pltpu.VMEM((rows, heads * cols, residues), F32),
                pltpu.VMEM((flat, chan), F32),
                pltpu.VMEM((rows * 8, cols), F32),
                pltpu.VMEM((planes, packed, chan), BF16),
                pltpu.VMEM((groups, per_owner, packed, chan), BF16),
                pltpu.VMEM((heads * cols, residues), F32),
                pltpu.VMEM((flat, chan), BF16),
                dma((2, planes // 2, CHUNKS)),
                dma((2, planes // 2, CHUNKS)),
                dma((planes,)),
                dma((groups, per_owner)),
                dma((groups,)),
                dma((groups,)),
                dma((planes,)),
                dma((planes,)),
                dma((groups,)),
                dma((groups,)),
            ],
            compiler_params=pltpu.CompilerParams(
                collective_id=0, has_side_effects=True, vmem_limit_bytes=56 * 1024 * 1024
            ),
            name="pair_update",
        )(*operands)

    placed = (P(("parts", "row"), ("col", "sub"), None), P("parts")) + (P(),) * 9
    return jax.shard_map(
        body,
        mesh=mesh,
        in_specs=placed,
        out_specs=P(("parts", "row"), ("col", "sub"), None),
        check_vma=False,
    )
```

```python
import functools

import jax
import jax.numpy as jnp
from jax import lax
from jax.experimental import pallas as pl
from jax.experimental.pallas import tpu as pltpu
from jax.sharding import PartitionSpec as P

MESH = pl.DeviceIdType.MESH
EPSILON = 1e-05
MASK_PENALTY = 1000000000.0
F32 = jnp.float32
BF16 = jnp.bfloat16
CHUNKS = 4
LAG = 4
STRIDE = 4


def norm_last(values_in, gain):
    center = jnp.mean(values_in, axis=-1, keepdims=True)
    centered = values_in - center
    variance = jnp.mean(centered * centered, axis=-1, keepdims=True)
    return centered * lax.rsqrt(variance + EPSILON) * gain


def dot(a, b):
    return lax.dot_general(a, b, (((1,), (0,)), ((), ())), preferred_element_type=F32)


def dot_nt(a, b):
    return lax.dot_general(a, b, (((1,), (1,)), ((), ())), preferred_element_type=F32)


def one_hot(rows, cols, match):
    r = lax.broadcasted_iota(jnp.int32, (rows, cols), 0)
    c = lax.broadcasted_iota(jnp.int32, (rows, cols), 1)
    return jnp.where(match(r, c), 1.0, 0.0).astype(BF16)


def kernel(
    planes,
    chips,
    subs,
    heads,
    pair_ref,
    mask_ref,
    gain1_ref,
    w_in_ref,
    w_gate_ref,
    gain2_ref,
    w_tri_ref,
    gain3_ref,
    w_att_ref,
    w_bias_ref,
    w_out_ref,
    out_ref,
    right_buf,
    left_buf,
    normed_buf,
    weight_buf,
    part_buf,
    sum_buf,
    tmp_buf,
    tri_buf,
    att_buf,
    key_buf,
    value_buf,
    query_buf,
    gate_buf,
    score_buf,
    mid_buf,
    bias_rows,
    bias_z,
    bias_x,
    bias_buf,
    gated_buf,
    ring_send,
    ring_recv,
    first_send,
    hand_send,
    hand_recv,
    part_send,
    part_recv,
    att_send,
    att_pass,
    att_recv,
    bz_far,
    bz_near,
    bz_recv,
    bx_send,
    bx_recv,
):
    rows, cols, chan = pair_ref.shape
    groups = chips * subs
    flat = rows * cols
    per_owner = planes // groups
    residues = groups * cols
    z = lax.axis_index("row")
    x = lax.axis_index("col")
    core = lax.axis_index("sub")
    g = x * subs + core
    mate = 1 - core
    ahead = lax.rem(z + planes + 2 * core - 1, planes)
    upper = lax.rem(z + 1, planes)
    lower = lax.rem(z + planes - 1, planes)

    def in_plane(c):
        return {"col": c // subs, "sub": lax.rem(c, subs)}

    barrier = pltpu.get_barrier_semaphore()
    for other in (upper, lower):
        for s in range(subs):
            pl.semaphore_signal(
                barrier, inc=1, device_id={"row": other, "sub": s}, device_id_type=MESH
            )
    for d in range(1, groups):
        pl.semaphore_signal(
            barrier, inc=1, device_id=in_plane(lax.rem(g + d, groups)), device_id_type=MESH
        )

    pair = pair_ref[...].reshape(flat, chan)
    normed = norm_last(pair, gain1_ref[...]).astype(BF16)
    normed_buf[...] = normed
    residue_live = mask_ref[...].reshape(1, residues).astype(F32)
    live_rows_of = jnp.broadcast_to(residue_live, (chan, residues)).astype(BF16)
    live_rows = dot_nt(one_hot(16, residues, lambda r, c: c == r + z * rows), live_rows_of)
    live_cols = dot_nt(one_hot(cols, residues, lambda r, c: c == r + g * cols), live_rows_of)
    live = jnp.concatenate([live_rows[i : i + 1] * live_cols for i in range(rows)], axis=0)
    weight_buf[...] = w_in_ref[...].astype(F32)

    def weight(p):
        return weight_buf[pl.ds(p, chan, stride=4), :].astype(BF16)

    def factor(p):
        gate = dot(normed, weight(p))
        value = dot(normed, weight(p + 1))
        return (jax.nn.sigmoid(gate) * value * live).astype(BF16)

    right_buf[z, core] = factor(2).reshape(rows, cols, chan)
    pl.semaphore_wait(barrier, 2 * subs + groups - 1)

    chunk_rows = rows // CHUNKS
    half = planes // 2
    last = half - 1

    def piece(origin, part, chunk):
        return right_buf.at[origin, part, pl.ds(chunk * chunk_rows, chunk_rows)]

    def behind(step):
        return lax.rem(z + 2 * planes - (2 * core - 1) * (1 + step), planes)

    def beyond(step):
        return lax.rem(z + 2 * planes + (2 * core - 1) * (1 + step), planes)

    def first_copy(way, chunk):
        return pltpu.make_async_remote_copy(
            src_ref=piece(z, core, chunk),
            dst_ref=piece(z, core, chunk),
            send_sem=first_send.at[way, chunk],
            recv_sem=ring_recv.at[0, core, chunk],
            device_id={"row": upper if way else lower, "sub": way},
            device_id_type=MESH,
        )

    def ring_copy(step, part, chunk):
        return pltpu.make_async_remote_copy(
            src_ref=piece(behind(step), part, chunk),
            dst_ref=piece(behind(step), part, chunk),
            send_sem=ring_send.at[step, part, chunk],
            recv_sem=ring_recv.at[step + 1, part, chunk],
            device_id={"row": ahead},
            device_id_type=MESH,
        )

    def ring_wait(step, part, chunk):
        block = piece(behind(step), part, chunk)
        pltpu.make_async_remote_copy(
            src_ref=block,
            dst_ref=block,
            send_sem=ring_send.at[0, part, chunk],
            recv_sem=ring_recv.at[step, part, chunk],
            device_id={"row": ahead},
            device_id_type=MESH,
        ).wait_recv()

    def hand_copy(step, chunk):
        block = piece(behind(step), mate, chunk)
        return pltpu.make_async_remote_copy(
            src_ref=block,
            dst_ref=block,
            send_sem=hand_send.at[step, chunk],
            recv_sem=hand_recv.at[step, chunk],
            device_id={"sub": mate},
            device_id_type=MESH,
        )

    def hand_wait(step, chunk):
        block = piece(beyond(step), core, chunk)
        pltpu.make_async_remote_copy(
            src_ref=block,
            dst_ref=block,
            send_sem=hand_send.at[step, chunk],
            recv_sem=hand_recv.at[step, chunk],
            device_id={"sub": mate},
            device_id_type=MESH,
        ).wait_recv()

    for chunk in range(CHUNKS):
        for way in range(2):
            first_copy(way, chunk).start()

    left_buf[...] = factor(0).astype(F32).reshape(rows, cols, chan)

    def products(origin, chunk):
        for j in range(chunk * chunk_rows, (chunk + 1) * chunk_rows):
            right = right_buf[origin, core, j].astype(F32)
            part_buf[origin, j * rows : (j + 1) * rows, :] = jnp.sum(
                left_buf[...] * right[None], axis=1
            )

    def part_copy(origin):
        owner = origin // per_owner
        return pltpu.make_async_remote_copy(
            src_ref=part_buf.at[origin],
            dst_ref=sum_buf.at[g, lax.rem(origin, per_owner)],
            send_sem=part_send.at[origin],
            recv_sem=part_recv.at[g, lax.rem(origin, per_owner)],
            device_id=in_plane(owner),
            device_id_type=MESH,
        )

    def to_owner(origin):
        @pl.when(origin // per_owner != g)
        def _():
            part_copy(origin).start()

    for chunk in range(CHUNKS):
        products(z, chunk)
    to_owner(z)
    weight_buf[...] = w_att_ref[...].astype(F32)

    far_chunks = CHUNKS // 2
    far_base = (1 - core) * far_chunks

    def handed(step):
        origin = beyond(step)
        for chunk in range(CHUNKS):
            hand_wait(step, chunk)
            products(origin, chunk)
        to_owner(origin)

    def ring_step(step, carry):
        origin = behind(step)
        for chunk in range(CHUNKS):
            wanted = (step + 1 < last) | (chunk // far_chunks == 1 - core)
            for part in range(subs):
                ring_wait(step, part, chunk)

                @pl.when(wanted)
                def _():
                    ring_copy(step, part, chunk).start()

            hand_copy(step, chunk).start()
            products(origin, chunk)
        to_owner(origin)

        @pl.when(step >= LAG)
        def _():
            handed(step - LAG)

        return carry

    lax.fori_loop(0, last, ring_step, 0)

    def late_step(step, carry):
        handed(step)
        return carry

    far = lax.rem(z + half, planes)
    for k in range(far_chunks):
        for part in range(subs):
            ring_wait(last, part, far_base + k)
        hand_copy(last, far_base + k).start()
    lax.fori_loop(max(last - LAG, 0), last, late_step, 0)
    for k in range(far_chunks):
        hand_wait(last, core * far_chunks + k)
    for chunk in range(CHUNKS):
        products(far, chunk)
    to_owner(far)

    tri_gate = jax.nn.sigmoid(dot(normed_buf[...], w_gate_ref[...]))

    block = rows * rows
    for p in range(per_owner):
        total = part_buf[g * per_owner + p]
        for d in range(1, groups):
            c = lax.rem(g + d, groups)
            pltpu.make_async_remote_copy(
                src_ref=part_buf.at[p],
                dst_ref=sum_buf.at[c, p],
                send_sem=part_send.at[p],
                recv_sem=part_recv.at[c, p],
                device_id=in_plane(c),
                device_id_type=MESH,
            ).wait_recv()
            total = total + sum_buf[c, p]
        tmp_buf[p * block : (p + 1) * block, :] = total
    for i in range(rows):
        tri_buf[i * cols : (i + 1) * cols, :] = tmp_buf[pl.ds(i, cols, stride=rows), :]

    hidden = norm_last(tri_buf[...], gain2_ref[...]).astype(BF16)
    pair_mid = pair_ref[...].reshape(flat, chan) + tri_gate * dot(hidden, w_tri_ref[...])
    mid_buf[...] = pair_mid
    att = norm_last(pair_mid, gain3_ref[...]).astype(BF16)
    att_buf[g] = att.reshape(rows, cols, chan)

    w_bias = jnp.concatenate(
        [w_bias_ref[...].astype(F32), jnp.zeros((8 - heads, chan), F32)], axis=0
    ).astype(BF16)

    for j in range(rows):
        bias_rows[j * 8 : (j + 1) * 8, :] = dot_nt(w_bias, att[j * cols : (j + 1) * cols, :])
    packed_rows = bias_z.shape[1]
    half_rows = rows // 2
    stacked = bias_rows[...].astype(BF16)
    message = jnp.zeros((packed_rows, chan), F32)
    for q in range(2):
        pick = one_hot(
            packed_rows,
            rows * 8,
            lambda r, c: c == (q * half_rows + lax.rem(r, half_rows)) * 8 + r // half_rows,
        )
        spread = one_hot(cols, chan, lambda r, c: c == r + q * cols)
        message = message + dot(dot(pick, stacked).astype(BF16), spread)
    bias_z[z] = message.astype(BF16)

    hops = planes // STRIDE
    near = (1, planes - 1, 2)

    def bz_copy(source, target, sem):
        return pltpu.make_async_remote_copy(
            src_ref=bias_z.at[source],
            dst_ref=bias_z.at[source],
            send_sem=sem,
            recv_sem=bz_recv.at[source],
            device_id={"row": target},
            device_id_type=MESH,
        )

    def bz_wait(source):
        bz_copy(source, z, bz_far.at[0]).wait_recv()

    def bz_far_copy(m):
        return bz_copy(z, lax.rem(z + STRIDE * m, planes), bz_far.at[m])

    def bz_near_copy(m, n):
        source = lax.rem(z + STRIDE * m, planes)
        return bz_copy(source, lax.rem(z + near[n], planes), bz_near.at[m, n])

    by_distance = sorted(range(1, hops), key=lambda m: min(m, hops - m))

    def pass_bias(m):
        if m:
            bz_wait(lax.rem(z + STRIDE * m, planes))
        for n in range(len(near)):
            bz_near_copy(m, n).start()

    for m in reversed(by_distance):
        bz_far_copy(m).start()
    pass_bias(0)

    def att_copy(source, target, sem):
        return pltpu.make_async_remote_copy(
            src_ref=att_buf.at[source],
            dst_ref=att_buf.at[source],
            send_sem=sem,
            recv_sem=att_recv.at[source],
            device_id=target,
            device_id_type=MESH,
        )

    def att_across(d):
        return att_copy(g, {"col": lax.rem(x + d, chips)}, att_send.at[d])

    def att_over(d):
        return att_copy(lax.rem(x + d, chips) * subs + core, {"sub": mate}, att_pass.at[d])

    for d in sorted(range(1, chips), key=lambda d: -min(d, chips - d)):
        att_across(d).start()
    att_over(0).start()

    def att_weight(p):
        return weight_buf[pl.ds(p, chan, stride=4), :].astype(BF16)

    scale = (chan // heads) ** (-0.5)
    query_buf[...] = (dot(att, att_weight(0)) * scale).astype(BF16)
    gate_buf[...] = jax.nn.sigmoid(dot(att, att_weight(3)))
    key_weight, value_weight = att_weight(1), att_weight(2)

    def key_value(c):
        here = pl.ds(pl.multiple_of(c * cols, cols), cols)
        normed_rows = att_buf[c].reshape(flat, chan)
        key_buf[:, here, :] = dot(normed_rows, key_weight).astype(BF16).reshape(rows, cols, chan)
        value_buf[:, here, :] = (
            dot(normed_rows, value_weight).astype(BF16).reshape(rows, cols, chan)
        )

    def att_wait(c):
        att_copy(c, {"sub": mate}, att_pass.at[0]).wait_recv()

    def ring_sent(step, carry):
        for chunk in range(CHUNKS):
            wanted = (step + 1 < last) | (chunk // far_chunks == 1 - core)

            @pl.when(wanted)
            def _():
                for part in range(subs):
                    ring_copy(step, part, chunk).wait_send()

            hand_copy(step, chunk).wait_send()
        return carry

    def parts_sent(origin, carry):
        @pl.when(origin // per_owner != g)
        def _():
            part_copy(origin).wait_send()

        return carry

    lax.fori_loop(0, last, ring_sent, 0)
    for k in range(far_chunks):
        hand_copy(last, far_base + k).wait_send()
    for chunk in range(CHUNKS):
        for way in range(2):
            first_copy(way, chunk).wait_send()
    lax.fori_loop(0, planes, parts_sent, 0)

    key_value(g)
    waiting = list(by_distance)
    for d in [0] + sorted(range(1, chips), key=lambda d: min(d, chips - d)):
        if d:
            c = lax.rem(x + d, chips) * subs + core
            att_wait(c)
            att_over(d).start()
            key_value(c)
        c = lax.rem(x + d, chips) * subs + mate
        att_wait(c)
        key_value(c)
        if len(waiting) > 2:
            for m in waiting[:2]:
                pass_bias(m)
            waiting = waiting[2:]

    lane_head = lax.broadcasted_iota(jnp.int32, (cols, chan), 1) // (chan // heads)

    def raw_scores(i, carry):
        query = query_buf[pl.ds(pl.multiple_of(i * cols, cols), cols), :]
        stack = jnp.concatenate(
            [jnp.where(lane_head == h, query, jnp.zeros_like(query)) for h in range(heads)], axis=0
        )
        score_buf[i] = dot_nt(stack, key_buf[i])
        return carry

    lax.fori_loop(0, rows, raw_scores, 0, unroll=2)
    for m in waiting:
        pass_bias(m)

    def bx_copy(source, target):
        return pltpu.make_async_remote_copy(
            src_ref=bias_z.at[pl.ds(target * per_owner, per_owner)],
            dst_ref=bias_x.at[source],
            send_sem=bx_send.at[target],
            recv_sem=bx_recv.at[source],
            device_id=in_plane(target),
            device_id_type=MESH,
        )

    for d in range(groups):
        c = lax.rem(g + d, groups)
        for p in range(per_owner):
            source = c * per_owner + p

            @pl.when(lax.rem(source + planes - z, STRIDE) != 0)
            def _():
                bz_wait(source)

        if d:
            bx_copy(g, c).start()

    sums = [jnp.zeros((per_owner * packed_rows, residues), F32) for _ in range(2)]
    for d in range(groups):
        c = lax.rem(g + d, groups)
        if d:
            bx_copy(c, g).wait_recv()
            piece = bias_x[c]
        else:
            piece = bias_z[pl.ds(g * per_owner, per_owner)]
        piece = piece.reshape(per_owner * packed_rows, chan)
        for q in range(2):
            spread = one_hot(
                chan, residues, lambda r, k: (k - c * cols == r - q * cols) & (r >= q * cols) & (r < (q + 1) * cols)
            )
            sums[q] = sums[q] + dot(piece, spread)
    bias = jnp.zeros((heads * cols, residues), F32)
    for q in range(2):
        def match(r, c):
            h, j = r // cols, lax.rem(r, cols)
            p, j = j // rows, lax.rem(j, rows)
            return (j // half_rows == q) & (
                c == p * packed_rows + h * half_rows + lax.rem(j, half_rows)
            )

        bias = bias + dot(
            one_hot(heads * cols, per_owner * packed_rows, match), sums[q].astype(BF16)
        )
    bias_buf[...] = bias + (residue_live - 1.0) * MASK_PENALTY

    def attend(i, carry):
        scores = score_buf[i] + bias_buf[...]
        raised = jnp.exp(scores - jnp.max(scores, axis=-1, keepdims=True))
        weights = (raised * (1.0 / jnp.sum(raised, axis=-1, keepdims=True))).astype(BF16)
        mixed = dot(weights, value_buf[i])
        attended = jnp.zeros((cols, chan), F32)
        for h in range(heads):
            attended = jnp.where(lane_head == h, mixed[h * cols : (h + 1) * cols, :], attended)
        here = pl.ds(pl.multiple_of(i * cols, cols), cols)
        gated_buf[here, :] = (attended * gate_buf[here, :]).astype(BF16)
        return carry

    lax.fori_loop(0, rows, attend, 0, unroll=2)
    out_ref[...] = (mid_buf[...] + dot(gated_buf[...], w_out_ref[...])).reshape(rows, cols, chan)

    for m in range(hops):
        if m:
            bz_far_copy(m).wait_send()
        for n in range(len(near)):
            bz_near_copy(m, n).wait_send()
    for d in range(chips):
        if d:
            att_across(d).wait_send()
        att_over(d).wait_send()
    for d in range(1, groups):
        bx_copy(g, lax.rem(g + d, groups)).wait_send()


def solution(mesh):
    planes = mesh.shape["row"]
    subs = mesh.shape["sub"]
    chips = mesh.shape["col"]
    groups = chips * subs

    def body(
        pair,
        residue_mask,
        tri_norm_gain,
        tri_in_weight,
        tri_gate_weight,
        tri_out_norm_gain,
        tri_out_weight,
        att_norm_gain,
        att_proj_weight,
        att_bias_weight,
        att_out_weight,
    ):
        rows, cols, chan = pair.shape
        heads = att_bias_weight.shape[1]
        residues = residue_mask.shape[0]
        flat = rows * cols
        per_owner = planes // groups
        packed = heads * rows // 2
        vmem = pl.BlockSpec(memory_space=pltpu.VMEM)
        dma = pltpu.SemaphoreType.DMA
        operands = (
            pair,
            residue_mask,
            tri_norm_gain[None, :],
            tri_in_weight.reshape(-1, chan),
            tri_gate_weight,
            tri_out_norm_gain[None, :],
            tri_out_weight,
            att_norm_gain[None, :],
            att_proj_weight.reshape(-1, chan),
            att_bias_weight.T,
            att_out_weight,
        )
        return pl.pallas_call(
            functools.partial(kernel, planes, chips, subs, heads),
            out_shape=jax.ShapeDtypeStruct(pair.shape, F32),
            in_specs=[vmem] * len(operands),
            out_specs=vmem,
            scratch_shapes=[
                pltpu.VMEM((planes, subs, rows, cols, chan), BF16),
                pltpu.VMEM((rows, cols, chan), F32),
                pltpu.VMEM((flat, chan), BF16),
                pltpu.VMEM((4 * chan, chan), F32),
                pltpu.VMEM((planes, rows * rows, chan), F32),
                pltpu.VMEM((groups, per_owner, rows * rows, chan), F32),
                pltpu.VMEM((flat, chan), F32),
                pltpu.VMEM((flat, chan), F32),
                pltpu.VMEM((groups, rows, cols, chan), BF16),
                pltpu.VMEM((rows, residues, chan), BF16),
                pltpu.VMEM((rows, residues, chan), BF16),
                pltpu.VMEM((flat, chan), BF16),
                pltpu.VMEM((flat, chan), F32),
                pltpu.VMEM((rows, heads * cols, residues), F32),
                pltpu.VMEM((flat, chan), F32),
                pltpu.VMEM((rows * 8, cols), F32),
                pltpu.VMEM((planes, packed, chan), BF16),
                pltpu.VMEM((groups, per_owner, packed, chan), BF16),
                pltpu.VMEM((heads * cols, residues), F32),
                pltpu.VMEM((flat, chan), BF16),
                dma((planes // 2, subs, CHUNKS)),
                dma((planes // 2, subs, CHUNKS)),
                dma((2, CHUNKS)),
                dma((planes // 2, CHUNKS)),
                dma((planes // 2, CHUNKS)),
                dma((planes,)),
                dma((groups, per_owner)),
                dma((chips,)),
                dma((chips,)),
                dma((groups,)),
                dma((planes // STRIDE,)),
                dma((planes // STRIDE, 3)),
                dma((planes,)),
                dma((groups,)),
                dma((groups,)),
            ],
            compiler_params=pltpu.CompilerParams(
                collective_id=0, has_side_effects=True, vmem_limit_bytes=56 * 1024 * 1024
            ),
            name="pair_update",
        )(*operands)

    placed = (P(("parts", "row"), ("col", "sub"), None), P("parts")) + (P(),) * 9
    return jax.shard_map(
        body,
        mesh=mesh,
        in_specs=placed,
        out_specs=P(("parts", "row"), ("col", "sub"), None),
        check_vma=False,
    )
```

```python
import functools

import jax
import jax.numpy as jnp
from jax import lax
from jax.experimental import pallas as pl
from jax.experimental.pallas import tpu as pltpu
from jax.sharding import PartitionSpec as P

MESH = pl.DeviceIdType.MESH
EPSILON = 1e-05
MASK_PENALTY = 1000000000.0
F32 = jnp.float32
BF16 = jnp.bfloat16
CHUNKS = 4
STRIDE = 4


def norm_last(values_in, gain):
    center = jnp.mean(values_in, axis=-1, keepdims=True)
    centered = values_in - center
    variance = jnp.mean(centered * centered, axis=-1, keepdims=True)
    return centered * lax.rsqrt(variance + EPSILON) * gain


def dot(a, b):
    return lax.dot_general(a, b, (((1,), (0,)), ((), ())), preferred_element_type=F32)


def dot_nt(a, b):
    return lax.dot_general(a, b, (((1,), (1,)), ((), ())), preferred_element_type=F32)


def one_hot(rows, cols, match):
    r = lax.broadcasted_iota(jnp.int32, (rows, cols), 0)
    c = lax.broadcasted_iota(jnp.int32, (rows, cols), 1)
    return jnp.where(match(r, c), 1.0, 0.0).astype(BF16)


def kernel(
    planes,
    chips,
    subs,
    heads,
    pair_ref,
    mask_ref,
    gain1_ref,
    w_in_ref,
    w_gate_ref,
    gain2_ref,
    w_tri_ref,
    gain3_ref,
    w_att_ref,
    w_bias_ref,
    w_out_ref,
    out_ref,
    right_buf,
    left_here,
    left_buf,
    normed_buf,
    weight_buf,
    part_buf,
    sum_buf,
    tmp_buf,
    tri_buf,
    att_buf,
    key_buf,
    value_buf,
    query_buf,
    gate_buf,
    score_buf,
    mid_buf,
    bias_rows,
    bias_z,
    bias_x,
    bias_buf,
    gated_buf,
    ring_send,
    ring_recv,
    first_send,
    mate_send,
    mate_recv,
    mate_done,
    part_send,
    part_recv,
    att_send,
    att_pass,
    att_recv,
    bz_far,
    bz_near,
    bz_recv,
    bx_send,
    bx_recv,
):
    rows, cols, chan = pair_ref.shape
    groups = chips * subs
    flat = rows * cols
    per_owner = planes // groups
    residues = groups * cols
    z = lax.axis_index("row")
    x = lax.axis_index("col")
    core = lax.axis_index("sub")
    g = x * subs + core
    mate = 1 - core
    ahead = lax.rem(z + planes + 2 * core - 1, planes)
    upper = lax.rem(z + 1, planes)
    lower = lax.rem(z + planes - 1, planes)

    def in_plane(c):
        return {"col": c // subs, "sub": lax.rem(c, subs)}

    barrier = pltpu.get_barrier_semaphore()
    for other in (upper, lower):
        for s in range(subs):
            pl.semaphore_signal(
                barrier, inc=1, device_id={"row": other, "sub": s}, device_id_type=MESH
            )
    for d in range(1, groups):
        pl.semaphore_signal(
            barrier, inc=1, device_id=in_plane(lax.rem(g + d, groups)), device_id_type=MESH
        )

    pair = pair_ref[...].reshape(flat, chan)
    normed = norm_last(pair, gain1_ref[...]).astype(BF16)
    normed_buf[...] = normed
    residue_live = mask_ref[...].reshape(1, residues).astype(F32)
    live_rows_of = jnp.broadcast_to(residue_live, (chan, residues)).astype(BF16)
    live_rows = dot_nt(one_hot(16, residues, lambda r, c: c == r + z * rows), live_rows_of)
    live_cols = dot_nt(one_hot(cols, residues, lambda r, c: c == r + g * cols), live_rows_of)
    live = jnp.concatenate([live_rows[i : i + 1] * live_cols for i in range(rows)], axis=0)
    weight_buf[...] = w_in_ref[...].astype(F32)

    def weight(p):
        return weight_buf[pl.ds(p, chan, stride=4), :].astype(BF16)

    def factor(p):
        gate = dot(normed, weight(p))
        value = dot(normed, weight(p + 1))
        return (jax.nn.sigmoid(gate) * value * live).astype(BF16)

    right_buf[z, core] = factor(2).reshape(rows, cols, chan)
    pl.semaphore_wait(barrier, 2 * subs + groups - 1)

    chunk_rows = rows // CHUNKS
    half = planes // 2
    last = half - 1

    def piece(origin, part, chunk):
        return right_buf.at[origin, part, pl.ds(chunk * chunk_rows, chunk_rows)]

    def behind(step):
        return lax.rem(z + 2 * planes - (2 * core - 1) * (1 + step), planes)

    def first_copy(way, chunk):
        return pltpu.make_async_remote_copy(
            src_ref=piece(z, core, chunk),
            dst_ref=piece(z, core, chunk),
            send_sem=first_send.at[way, chunk],
            recv_sem=ring_recv.at[0, core, chunk],
            device_id={"row": upper if way else lower, "sub": way},
            device_id_type=MESH,
        )

    def ring_copy(step, part, chunk):
        return pltpu.make_async_remote_copy(
            src_ref=piece(behind(step), part, chunk),
            dst_ref=piece(behind(step), part, chunk),
            send_sem=ring_send.at[step, part, chunk],
            recv_sem=ring_recv.at[step + 1, part, chunk],
            device_id={"row": ahead},
            device_id_type=MESH,
        )

    def ring_wait(step, part, chunk):
        block = piece(behind(step), part, chunk)
        pltpu.make_async_remote_copy(
            src_ref=block,
            dst_ref=block,
            send_sem=ring_send.at[0, part, chunk],
            recv_sem=ring_recv.at[step, part, chunk],
            device_id={"row": ahead},
            device_id_type=MESH,
        ).wait_recv()

    def mate_copy(ref, k):
        return pltpu.make_async_remote_copy(
            src_ref=ref,
            dst_ref=ref,
            send_sem=mate_send.at[k],
            recv_sem=mate_recv.at[k],
            device_id={"sub": mate},
            device_id_type=MESH,
        )

    for chunk in range(CHUNKS):
        for way in range(2):
            first_copy(way, chunk).start()
    mate_copy(right_buf.at[z, core], 0).start()
    left = factor(0)
    left_here[core] = left.reshape(rows, cols, chan)
    mate_copy(left_here.at[core], 1).start()
    left_buf[core] = left.astype(F32).reshape(rows, cols, chan)
    weight_buf[...] = w_att_ref[...].astype(F32)

    side = 1 - core
    half_chunks = CHUNKS // 2

    def products(origin, h, first, chunk):
        for j in range(chunk_rows):
            total = jnp.zeros((rows, chan), F32)
            for part in range(subs):
                right = right_buf[origin, part, (first + chunk) * chunk_rows + j].astype(F32)
                total = total + jnp.sum(left_buf[part] * right[None], axis=1)
            row = (chunk * chunk_rows + j) * rows
            part_buf[origin, h, row : row + rows, :] = total

    def part_copy(origin, h):
        return pltpu.make_async_remote_copy(
            src_ref=part_buf.at[origin, h],
            dst_ref=sum_buf.at[x, lax.rem(origin, per_owner), h],
            send_sem=part_send.at[origin, h],
            recv_sem=part_recv.at[x, lax.rem(origin, per_owner), h],
            device_id=in_plane(origin // per_owner),
            device_id_type=MESH,
        )

    def to_owner(origin, h):
        mine = origin // per_owner == g

        @pl.when(jnp.logical_not(mine))
        def _():
            part_copy(origin, h).start()

        @pl.when(mine)
        def _():
            sum_buf[x, lax.rem(origin, per_owner), h] = part_buf[origin, h]

    def takes(origin, h):
        gap = lax.rem(z + planes - origin, planes)
        shared = (gap == 0) | (gap == half)
        return (shared & (side == h)) | (jnp.logical_not(shared) & ((gap < half) == (core == 1)))

    mate_copy(right_buf.at[z, mate], 0).wait_recv()
    mate_copy(left_here.at[mate], 1).wait_recv()
    left_buf[mate] = left_here[mate].astype(F32)
    for chunk in range(half_chunks):
        products(z, side, side * half_chunks, chunk)
    to_owner(z, side)

    def ring_step(step, carry):
        origin = behind(step)
        for chunk in range(CHUNKS):
            wanted = (step + 1 < last) | (chunk // half_chunks == side)
            for part in range(subs):
                ring_wait(step, part, chunk)

                @pl.when(wanted)
                def _():
                    ring_copy(step, part, chunk).start()

            h = chunk // half_chunks
            products(origin, h, h * half_chunks, chunk % half_chunks)
            if chunk % half_chunks == half_chunks - 1:
                to_owner(origin, h)
        return carry

    lax.fori_loop(0, last, ring_step, 0)
    far = lax.rem(z + half, planes)
    for k in range(half_chunks):
        for part in range(subs):
            ring_wait(last, part, side * half_chunks + k)
        products(far, side, side * half_chunks, k)
    to_owner(far, side)
    pl.semaphore_signal(mate_done, inc=1, device_id={"sub": mate}, device_id_type=MESH)

    tri_gate = jax.nn.sigmoid(dot(normed_buf[...], w_gate_ref[...]))

    block = rows * rows
    for p in range(per_owner):
        origin = g * per_owner + p
        for h in range(2):
            for d in range(chips):
                chip = lax.rem(x + d, chips)

                @pl.when(jnp.logical_not(takes(origin, h)) if d == 0 else chip >= 0)
                def _():
                    pltpu.make_async_remote_copy(
                        src_ref=part_buf.at[0, h],
                        dst_ref=sum_buf.at[chip, p, h],
                        send_sem=part_send.at[0, h],
                        recv_sem=part_recv.at[chip, p, h],
                        device_id=in_plane(g),
                        device_id_type=MESH,
                    ).wait_recv()

            total = sum_buf[0, p, h]
            for chip in range(1, chips):
                total = total + sum_buf[chip, p, h]
            at = p * block + h * (block // 2)
            tmp_buf[at : at + block // 2, :] = total
    for i in range(rows):
        tri_buf[i * cols : (i + 1) * cols, :] = tmp_buf[pl.ds(i, cols, stride=rows), :]

    hidden = norm_last(tri_buf[...], gain2_ref[...]).astype(BF16)
    pair_mid = pair_ref[...].reshape(flat, chan) + tri_gate * dot(hidden, w_tri_ref[...])
    mid_buf[...] = pair_mid
    att = norm_last(pair_mid, gain3_ref[...]).astype(BF16)
    att_buf[g] = att.reshape(rows, cols, chan)

    w_bias = jnp.concatenate(
        [w_bias_ref[...].astype(F32), jnp.zeros((8 - heads, chan), F32)], axis=0
    ).astype(BF16)

    for j in range(rows):
        bias_rows[j * 8 : (j + 1) * 8, :] = dot_nt(w_bias, att[j * cols : (j + 1) * cols, :])
    packed_rows = bias_z.shape[1]
    half_rows = rows // 2
    stacked = bias_rows[...].astype(BF16)
    message = jnp.zeros((packed_rows, chan), F32)
    for q in range(2):
        pick = one_hot(
            packed_rows,
            rows * 8,
            lambda r, c: c == (q * half_rows + lax.rem(r, half_rows)) * 8 + r // half_rows,
        )
        spread = one_hot(cols, chan, lambda r, c: c == r + q * cols)
        message = message + dot(dot(pick, stacked).astype(BF16), spread)
    bias_z[z] = message.astype(BF16)

    hops = planes // STRIDE
    near = (1, planes - 1, 2)

    def bz_copy(source, target, sem):
        return pltpu.make_async_remote_copy(
            src_ref=bias_z.at[source],
            dst_ref=bias_z.at[source],
            send_sem=sem,
            recv_sem=bz_recv.at[source],
            device_id={"row": target},
            device_id_type=MESH,
        )

    def bz_wait(source):
        bz_copy(source, z, bz_far.at[0]).wait_recv()

    def bz_far_copy(m):
        return bz_copy(z, lax.rem(z + STRIDE * m, planes), bz_far.at[m])

    def bz_near_copy(m, n):
        source = lax.rem(z + STRIDE * m, planes)
        return bz_copy(source, lax.rem(z + near[n], planes), bz_near.at[m, n])

    by_distance = sorted(range(1, hops), key=lambda m: min(m, hops - m))

    def pass_bias(m):
        if m:
            bz_wait(lax.rem(z + STRIDE * m, planes))
        for n in range(len(near)):
            bz_near_copy(m, n).start()

    pl.semaphore_wait(mate_done, 1)
    for m in reversed(by_distance):
        bz_far_copy(m).start()
    pass_bias(0)

    def att_copy(source, target, sem):
        return pltpu.make_async_remote_copy(
            src_ref=att_buf.at[source],
            dst_ref=att_buf.at[source],
            send_sem=sem,
            recv_sem=att_recv.at[source],
            device_id=target,
            device_id_type=MESH,
        )

    def att_across(d):
        return att_copy(g, {"col": lax.rem(x + d, chips)}, att_send.at[d])

    def att_over(d):
        return att_copy(lax.rem(x + d, chips) * subs + core, {"sub": mate}, att_pass.at[d])

    for d in sorted(range(1, chips), key=lambda d: -min(d, chips - d)):
        att_across(d).start()
    att_over(0).start()

    def att_weight(p):
        return weight_buf[pl.ds(p, chan, stride=4), :].astype(BF16)

    scale = (chan // heads) ** (-0.5)
    query_buf[...] = (dot(att, att_weight(0)) * scale).astype(BF16)
    gate_buf[...] = jax.nn.sigmoid(dot(att, att_weight(3)))
    key_weight, value_weight = att_weight(1), att_weight(2)

    def key_value(c):
        here = pl.ds(pl.multiple_of(c * cols, cols), cols)
        normed_rows = att_buf[c].reshape(flat, chan)
        key_buf[:, here, :] = dot(normed_rows, key_weight).astype(BF16).reshape(rows, cols, chan)
        value_buf[:, here, :] = (
            dot(normed_rows, value_weight).astype(BF16).reshape(rows, cols, chan)
        )

    def att_wait(c):
        att_copy(c, {"sub": mate}, att_pass.at[0]).wait_recv()

    def ring_sent(step, carry):
        for chunk in range(CHUNKS):
            wanted = (step + 1 < last) | (chunk // half_chunks == side)

            @pl.when(wanted)
            def _():
                for part in range(subs):
                    ring_copy(step, part, chunk).wait_send()

        return carry

    def parts_sent(origin, carry):
        for h in range(2):

            @pl.when(takes(origin, h) & (origin // per_owner != g))
            def _():
                part_copy(origin, h).wait_send()

        return carry

    lax.fori_loop(0, last, ring_sent, 0)
    for chunk in range(CHUNKS):
        for way in range(2):
            first_copy(way, chunk).wait_send()
    mate_copy(right_buf.at[z, core], 0).wait_send()
    mate_copy(left_here.at[core], 1).wait_send()
    lax.fori_loop(0, planes, parts_sent, 0)

    key_value(g)
    waiting = list(by_distance)
    for d in [0] + sorted(range(1, chips), key=lambda d: min(d, chips - d)):
        if d:
            c = lax.rem(x + d, chips) * subs + core
            att_wait(c)
            att_over(d).start()
            key_value(c)
        c = lax.rem(x + d, chips) * subs + mate
        att_wait(c)
        key_value(c)
        if len(waiting) > 2:
            for m in waiting[:2]:
                pass_bias(m)
            waiting = waiting[2:]

    lane_head = lax.broadcasted_iota(jnp.int32, (cols, chan), 1) // (chan // heads)

    def raw_scores(i, carry):
        query = query_buf[pl.ds(pl.multiple_of(i * cols, cols), cols), :]
        stack = jnp.concatenate(
            [jnp.where(lane_head == h, query, jnp.zeros_like(query)) for h in range(heads)], axis=0
        )
        score_buf[i] = dot_nt(stack, key_buf[i])
        return carry

    lax.fori_loop(0, rows, raw_scores, 0, unroll=2)
    for m in waiting:
        pass_bias(m)

    def bx_copy(source, target):
        return pltpu.make_async_remote_copy(
            src_ref=bias_z.at[pl.ds(target * per_owner, per_owner)],
            dst_ref=bias_x.at[source],
            send_sem=bx_send.at[target],
            recv_sem=bx_recv.at[source],
            device_id=in_plane(target),
            device_id_type=MESH,
        )

    for d in range(groups):
        c = lax.rem(g + d, groups)
        for p in range(per_owner):
            source = c * per_owner + p

            @pl.when(lax.rem(source + planes - z, STRIDE) != 0)
            def _():
                bz_wait(source)

        if d:
            bx_copy(g, c).start()

    sums = [jnp.zeros((per_owner * packed_rows, residues), F32) for _ in range(2)]
    for d in range(groups):
        c = lax.rem(g + d, groups)
        if d:
            bx_copy(c, g).wait_recv()
            piece = bias_x[c]
        else:
            piece = bias_z[pl.ds(g * per_owner, per_owner)]
        piece = piece.reshape(per_owner * packed_rows, chan)
        for q in range(2):
            spread = one_hot(
                chan, residues, lambda r, k: (k - c * cols == r - q * cols) & (r >= q * cols) & (r < (q + 1) * cols)
            )
            sums[q] = sums[q] + dot(piece, spread)
    bias = jnp.zeros((heads * cols, residues), F32)
    for q in range(2):
        def match(r, c):
            h, j = r // cols, lax.rem(r, cols)
            p, j = j // rows, lax.rem(j, rows)
            return (j // half_rows == q) & (
                c == p * packed_rows + h * half_rows + lax.rem(j, half_rows)
            )

        bias = bias + dot(
            one_hot(heads * cols, per_owner * packed_rows, match), sums[q].astype(BF16)
        )
    bias_buf[...] = bias + (residue_live - 1.0) * MASK_PENALTY

    def attend(i, carry):
        scores = score_buf[i] + bias_buf[...]
        raised = jnp.exp(scores - jnp.max(scores, axis=-1, keepdims=True))
        weights = (raised * (1.0 / jnp.sum(raised, axis=-1, keepdims=True))).astype(BF16)
        mixed = dot(weights, value_buf[i])
        attended = jnp.zeros((cols, chan), F32)
        for h in range(heads):
            attended = jnp.where(lane_head == h, mixed[h * cols : (h + 1) * cols, :], attended)
        here = pl.ds(pl.multiple_of(i * cols, cols), cols)
        gated_buf[here, :] = (attended * gate_buf[here, :]).astype(BF16)
        return carry

    lax.fori_loop(0, rows, attend, 0, unroll=2)
    out_ref[...] = (mid_buf[...] + dot(gated_buf[...], w_out_ref[...])).reshape(rows, cols, chan)

    for m in range(hops):
        if m:
            bz_far_copy(m).wait_send()
        for n in range(len(near)):
            bz_near_copy(m, n).wait_send()
    for d in range(chips):
        if d:
            att_across(d).wait_send()
        att_over(d).wait_send()
    for d in range(1, groups):
        bx_copy(g, lax.rem(g + d, groups)).wait_send()


def solution(mesh):
    planes = mesh.shape["row"]
    subs = mesh.shape["sub"]
    chips = mesh.shape["col"]
    groups = chips * subs

    def body(
        pair,
        residue_mask,
        tri_norm_gain,
        tri_in_weight,
        tri_gate_weight,
        tri_out_norm_gain,
        tri_out_weight,
        att_norm_gain,
        att_proj_weight,
        att_bias_weight,
        att_out_weight,
    ):
        rows, cols, chan = pair.shape
        heads = att_bias_weight.shape[1]
        residues = residue_mask.shape[0]
        flat = rows * cols
        per_owner = planes // groups
        packed = heads * rows // 2
        vmem = pl.BlockSpec(memory_space=pltpu.VMEM)
        dma = pltpu.SemaphoreType.DMA
        operands = (
            pair,
            residue_mask,
            tri_norm_gain[None, :],
            tri_in_weight.reshape(-1, chan),
            tri_gate_weight,
            tri_out_norm_gain[None, :],
            tri_out_weight,
            att_norm_gain[None, :],
            att_proj_weight.reshape(-1, chan),
            att_bias_weight.T,
            att_out_weight,
        )
        return pl.pallas_call(
            functools.partial(kernel, planes, chips, subs, heads),
            out_shape=jax.ShapeDtypeStruct(pair.shape, F32),
            in_specs=[vmem] * len(operands),
            out_specs=vmem,
            scratch_shapes=[
                pltpu.VMEM((planes, subs, rows, cols, chan), BF16),
                pltpu.VMEM((subs, rows, cols, chan), BF16),
                pltpu.VMEM((subs, rows, cols, chan), F32),
                pltpu.VMEM((flat, chan), BF16),
                pltpu.VMEM((4 * chan, chan), F32),
                pltpu.VMEM((planes, 2, rows * rows // 2, chan), F32),
                pltpu.VMEM((chips, per_owner, 2, rows * rows // 2, chan), F32),
                pltpu.VMEM((flat, chan), F32),
                pltpu.VMEM((flat, chan), F32),
                pltpu.VMEM((groups, rows, cols, chan), BF16),
                pltpu.VMEM((rows, residues, chan), BF16),
                pltpu.VMEM((rows, residues, chan), BF16),
                pltpu.VMEM((flat, chan), BF16),
                pltpu.VMEM((flat, chan), F32),
                pltpu.VMEM((rows, heads * cols, residues), F32),
                pltpu.VMEM((flat, chan), F32),
                pltpu.VMEM((rows * 8, cols), F32),
                pltpu.VMEM((planes, packed, chan), BF16),
                pltpu.VMEM((groups, per_owner, packed, chan), BF16),
                pltpu.VMEM((heads * cols, residues), F32),
                pltpu.VMEM((flat, chan), BF16),
                dma((planes // 2, subs, CHUNKS)),
                dma((planes // 2, subs, CHUNKS)),
                dma((2, CHUNKS)),
                dma((2,)),
                dma((2,)),
                pltpu.SemaphoreType.REGULAR,
                dma((planes, 2)),
                dma((chips, per_owner, 2)),
                dma((chips,)),
                dma((chips,)),
                dma((groups,)),
                dma((planes // STRIDE,)),
                dma((planes // STRIDE, 3)),
                dma((planes,)),
                dma((groups,)),
                dma((groups,)),
            ],
            compiler_params=pltpu.CompilerParams(
                collective_id=0, has_side_effects=True, vmem_limit_bytes=56 * 1024 * 1024
            ),
            name="pair_update",
        )(*operands)

    placed = (P(("parts", "row"), ("col", "sub"), None), P("parts")) + (P(),) * 9
    return jax.shard_map(
        body,
        mesh=mesh,
        in_specs=placed,
        out_specs=P(("parts", "row"), ("col", "sub"), None),
        check_vma=False,
    )
```

```python
import functools

import jax
import jax.numpy as jnp
from jax import lax
from jax.experimental import pallas as pl
from jax.experimental.pallas import tpu as pltpu
from jax.sharding import PartitionSpec as P

MESH = pl.DeviceIdType.MESH
EPSILON = 1e-05
MASK_PENALTY = 1000000000.0
F32 = jnp.float32
BF16 = jnp.bfloat16
CHUNKS = 4
STRIDE = 4


def norm_last(values_in, gain):
    center = jnp.mean(values_in, axis=-1, keepdims=True)
    centered = values_in - center
    variance = jnp.mean(centered * centered, axis=-1, keepdims=True)
    return centered * lax.rsqrt(variance + EPSILON) * gain


def dot(a, b):
    return lax.dot_general(a, b, (((1,), (0,)), ((), ())), preferred_element_type=F32)


def dot_nt(a, b):
    return lax.dot_general(a, b, (((1,), (1,)), ((), ())), preferred_element_type=F32)


def one_hot(rows, cols, match):
    r = lax.broadcasted_iota(jnp.int32, (rows, cols), 0)
    c = lax.broadcasted_iota(jnp.int32, (rows, cols), 1)
    return jnp.where(match(r, c), 1.0, 0.0).astype(BF16)


def kernel(
    planes,
    chips,
    subs,
    heads,
    pair_ref,
    mask_ref,
    gain1_ref,
    w_in_ref,
    w_gate_ref,
    gain2_ref,
    w_tri_ref,
    gain3_ref,
    w_att_ref,
    w_bias_ref,
    w_out_ref,
    out_ref,
    right_buf,
    left_here,
    left_buf,
    normed_buf,
    weight_buf,
    stage_buf,
    part_buf,
    sum_buf,
    tmp_buf,
    tri_buf,
    att_buf,
    key_buf,
    value_buf,
    query_buf,
    gate_buf,
    score_buf,
    mid_buf,
    bias_rows,
    bias_z,
    bias_x,
    bias_buf,
    gated_buf,
    ring_send,
    ring_recv,
    first_send,
    mate_send,
    mate_recv,
    mate_done,
    plane_done,
    part_send,
    part_recv,
    att_send,
    att_pass,
    att_recv,
    bz_far,
    bz_near,
    bz_recv,
    bx_recv,
):
    rows, cols, chan = pair_ref.shape
    groups = chips * subs
    flat = rows * cols
    per_owner = planes // groups
    residues = groups * cols
    z = lax.axis_index("row")
    x = lax.axis_index("col")
    core = lax.axis_index("sub")
    g = x * subs + core
    mate = 1 - core
    ahead = lax.rem(z + planes + 2 * core - 1, planes)
    upper = lax.rem(z + 1, planes)
    lower = lax.rem(z + planes - 1, planes)

    def in_plane(c):
        return {"col": c // subs, "sub": lax.rem(c, subs)}

    barrier = pltpu.get_barrier_semaphore()
    for other in (upper, lower):
        for s in range(subs):
            pl.semaphore_signal(
                barrier, inc=1, device_id={"row": other, "sub": s}, device_id_type=MESH
            )
    for d in range(1, groups):
        pl.semaphore_signal(
            barrier, inc=1, device_id=in_plane(lax.rem(g + d, groups)), device_id_type=MESH
        )

    pair = pair_ref[...].reshape(flat, chan)
    normed = norm_last(pair, gain1_ref[...]).astype(BF16)
    normed_buf[...] = normed
    residue_live = mask_ref[...].reshape(1, residues).astype(F32)
    live_rows_of = jnp.broadcast_to(residue_live, (chan, residues)).astype(BF16)
    live_rows = dot_nt(one_hot(16, residues, lambda r, c: c == r + z * rows), live_rows_of)
    live_cols = dot_nt(one_hot(cols, residues, lambda r, c: c == r + g * cols), live_rows_of)
    live = jnp.concatenate([live_rows[i : i + 1] * live_cols for i in range(rows)], axis=0)
    weight_buf[...] = w_in_ref[...].astype(F32)

    def weight(p):
        return weight_buf[pl.ds(p, chan, stride=4), :].astype(BF16)

    def factor(p):
        gate = dot(normed, weight(p))
        value = dot(normed, weight(p + 1))
        return (jax.nn.sigmoid(gate) * value * live).astype(BF16)

    right_buf[z, core] = factor(2).reshape(rows, cols, chan)
    pl.semaphore_wait(barrier, 2 * subs + groups - 1)

    chunk_rows = rows // CHUNKS
    half = planes // 2
    last = half - 1

    def piece(origin, part, chunk):
        return right_buf.at[origin, part, pl.ds(chunk * chunk_rows, chunk_rows)]

    def behind(step):
        return lax.rem(z + 2 * planes - (2 * core - 1) * (1 + step), planes)

    def first_copy(way, chunk):
        return pltpu.make_async_remote_copy(
            src_ref=piece(z, core, chunk),
            dst_ref=piece(z, core, chunk),
            send_sem=first_send.at[way, chunk],
            recv_sem=ring_recv.at[0, core, chunk],
            device_id={"row": upper if way else lower, "sub": way},
            device_id_type=MESH,
        )

    def ring_copy(step, part, chunk):
        return pltpu.make_async_remote_copy(
            src_ref=piece(behind(step), part, chunk),
            dst_ref=piece(behind(step), part, chunk),
            send_sem=ring_send.at[step, part, chunk],
            recv_sem=ring_recv.at[step + 1, part, chunk],
            device_id={"row": ahead},
            device_id_type=MESH,
        )

    def ring_wait(step, part, chunk):
        block = piece(behind(step), part, chunk)
        pltpu.make_async_remote_copy(
            src_ref=block,
            dst_ref=block,
            send_sem=ring_send.at[0, part, chunk],
            recv_sem=ring_recv.at[step, part, chunk],
            device_id={"row": ahead},
            device_id_type=MESH,
        ).wait_recv()

    def mate_copy(ref, k):
        return pltpu.make_async_remote_copy(
            src_ref=ref,
            dst_ref=ref,
            send_sem=mate_send.at[k],
            recv_sem=mate_recv.at[k],
            device_id={"sub": mate},
            device_id_type=MESH,
        )

    for chunk in range(CHUNKS):
        for way in range(2):
            first_copy(way, chunk).start()
    mate_copy(right_buf.at[z, core], 0).start()
    left = factor(0)
    left_here[core] = left.reshape(rows, cols, chan)
    mate_copy(left_here.at[core], 1).start()
    left_buf[core] = left.astype(F32).reshape(rows, cols, chan)
    weight_buf[...] = w_att_ref[...].astype(F32)

    side = 1 - core
    half_chunks = CHUNKS // 2

    def products(origin, first, chunk):
        for j in range(chunk_rows):
            total = jnp.zeros((rows, chan), F32)
            for part in range(subs):
                right = right_buf[origin, part, (first + chunk) * chunk_rows + j].astype(F32)
                total = total + jnp.sum(left_buf[part] * right[None], axis=1)
            row = (chunk * chunk_rows + j) * rows
            stage_buf[row : row + rows, :] = total

    def part_copy(origin, h):
        return pltpu.make_async_remote_copy(
            src_ref=part_buf.at[origin, h],
            dst_ref=sum_buf.at[x, lax.rem(origin, per_owner), h],
            send_sem=part_send.at[origin, h],
            recv_sem=part_recv.at[x, lax.rem(origin, per_owner), h],
            device_id=in_plane(origin // per_owner),
            device_id_type=MESH,
        )

    def to_owner(origin, h):
        mine = origin // per_owner == g

        @pl.when(jnp.logical_not(mine))
        def _():
            part_buf[origin, h] = stage_buf[...]
            part_copy(origin, h).start()

        @pl.when(mine)
        def _():
            sum_buf[x, lax.rem(origin, per_owner), h] = stage_buf[...]

    def takes(origin, h):
        gap = lax.rem(z + planes - origin, planes)
        shared = (gap == 0) | (gap == half)
        return (shared & (side == h)) | (jnp.logical_not(shared) & ((gap < half) == (core == 1)))

    mate_copy(right_buf.at[z, mate], 0).wait_recv()
    mate_copy(left_here.at[mate], 1).wait_recv()
    left_buf[mate] = left_here[mate].astype(F32)
    for chunk in range(half_chunks):
        products(z, side * half_chunks, chunk)
    to_owner(z, side)

    def ring_step(step, carry):
        origin = behind(step)
        for chunk in range(CHUNKS):
            wanted = (step + 1 < last) | (chunk // half_chunks == side)
            for part in range(subs):
                ring_wait(step, part, chunk)

                @pl.when(wanted)
                def _():
                    ring_copy(step, part, chunk).start()

            h = chunk // half_chunks
            products(origin, h * half_chunks, chunk % half_chunks)
            if chunk % half_chunks == half_chunks - 1:
                to_owner(origin, h)
        return carry

    lax.fori_loop(0, last, ring_step, 0)
    far = lax.rem(z + half, planes)
    for k in range(half_chunks):
        for part in range(subs):
            ring_wait(last, part, side * half_chunks + k)
        products(far, side * half_chunks, k)
    to_owner(far, side)
    pl.semaphore_signal(mate_done, inc=1, device_id={"sub": mate}, device_id_type=MESH)
    for d in range(1, groups):
        pl.semaphore_signal(
            plane_done, inc=1, device_id=in_plane(lax.rem(g + d, groups)), device_id_type=MESH
        )

    tri_gate = jax.nn.sigmoid(dot(normed_buf[...], w_gate_ref[...]))

    block = rows * rows
    for p in range(per_owner):
        origin = g * per_owner + p
        for h in range(2):
            for d in range(chips):
                chip = lax.rem(x + d, chips)

                @pl.when(jnp.logical_not(takes(origin, h)) if d == 0 else chip >= 0)
                def _():
                    pltpu.make_async_remote_copy(
                        src_ref=part_buf.at[0, h],
                        dst_ref=sum_buf.at[chip, p, h],
                        send_sem=part_send.at[0, h],
                        recv_sem=part_recv.at[chip, p, h],
                        device_id=in_plane(g),
                        device_id_type=MESH,
                    ).wait_recv()

            total = sum_buf[0, p, h]
            for chip in range(1, chips):
                total = total + sum_buf[chip, p, h]
            at = p * block + h * (block // 2)
            tmp_buf[at : at + block // 2, :] = total
    for i in range(rows):
        tri_buf[i * cols : (i + 1) * cols, :] = tmp_buf[pl.ds(i, cols, stride=rows), :]

    hidden = norm_last(tri_buf[...], gain2_ref[...]).astype(BF16)
    pair_mid = pair_ref[...].reshape(flat, chan) + tri_gate * dot(hidden, w_tri_ref[...])
    mid_buf[...] = pair_mid
    att = norm_last(pair_mid, gain3_ref[...]).astype(BF16)
    att_buf[g] = att.reshape(rows, cols, chan)

    w_bias = jnp.concatenate(
        [w_bias_ref[...].astype(F32), jnp.zeros((8 - heads, chan), F32)], axis=0
    ).astype(BF16)

    for j in range(rows):
        bias_rows[j * 8 : (j + 1) * 8, :] = dot_nt(w_bias, att[j * cols : (j + 1) * cols, :])
    packed_rows = bias_z.shape[1]
    half_rows = rows // 2
    stacked = bias_rows[...].astype(BF16)
    message = jnp.zeros((packed_rows, chan), F32)
    for q in range(2):
        pick = one_hot(
            packed_rows,
            rows * 8,
            lambda r, c: c == (q * half_rows + lax.rem(r, half_rows)) * 8 + r // half_rows,
        )
        spread = one_hot(cols, chan, lambda r, c: c == r + q * cols)
        message = message + dot(dot(pick, stacked).astype(BF16), spread)
    bias_z[z] = message.astype(BF16)

    hops = planes // STRIDE
    near = (1, planes - 1, 2, 0)

    def bz_copy(source, target, sem):
        return pltpu.make_async_remote_copy(
            src_ref=bias_z.at[source],
            dst_ref=bias_z.at[source],
            send_sem=sem,
            recv_sem=bz_recv.at[source],
            device_id={"row": target},
            device_id_type=MESH,
        )

    def bz_wait(source):
        bz_copy(source, z, bz_far.at[0]).wait_recv()

    def bz_far_copy(m):
        return bz_copy(z, lax.rem(z + STRIDE * m, planes), bz_far.at[m])

    def bz_near_copy(m, n):
        source = lax.rem(z + STRIDE * m, planes)
        return pltpu.make_async_remote_copy(
            src_ref=bias_z.at[source],
            dst_ref=bias_x.at[g, lax.rem(source, per_owner)],
            send_sem=bz_near.at[m, n],
            recv_sem=bx_recv.at[g, lax.rem(source, per_owner)],
            device_id={"row": lax.rem(z + near[n], planes), **in_plane(source // per_owner)},
            device_id_type=MESH,
        )

    def leaves(m, n):
        return (lax.rem(z + STRIDE * m, planes) // per_owner != g) if near[n] == 0 else g >= 0

    by_distance = sorted(range(1, hops), key=lambda m: min(m, hops - m))

    def pass_bias(m):
        if m:
            bz_wait(lax.rem(z + STRIDE * m, planes))
        for n in range(len(near)):

            @pl.when(leaves(m, n))
            def _():
                bz_near_copy(m, n).start()

        source = lax.rem(z + STRIDE * m, planes)

        @pl.when(source // per_owner == g)
        def _():
            bias_x[g, lax.rem(source, per_owner)] = bias_z[source]

    pl.semaphore_wait(mate_done, 1)
    for m in reversed(by_distance):
        bz_far_copy(m).start()
    pl.semaphore_wait(plane_done, groups - 1)
    pass_bias(0)

    def att_copy(source, target, sem):
        return pltpu.make_async_remote_copy(
            src_ref=att_buf.at[source],
            dst_ref=att_buf.at[source],
            send_sem=sem,
            recv_sem=att_recv.at[source],
            device_id=target,
            device_id_type=MESH,
        )

    def att_across(d):
        return att_copy(g, {"col": lax.rem(x + d, chips)}, att_send.at[d])

    def att_over(d):
        return att_copy(lax.rem(x + d, chips) * subs + core, {"sub": mate}, att_pass.at[d])

    for d in sorted(range(1, chips), key=lambda d: -min(d, chips - d)):
        att_across(d).start()
    att_over(0).start()

    def att_weight(p):
        return weight_buf[pl.ds(p, chan, stride=4), :].astype(BF16)

    scale = (chan // heads) ** (-0.5)
    query_buf[...] = (dot(att, att_weight(0)) * scale).astype(BF16)
    gate_buf[...] = jax.nn.sigmoid(dot(att, att_weight(3)))
    key_weight, value_weight = att_weight(1), att_weight(2)

    def key_value(c):
        here = pl.ds(pl.multiple_of(c * cols, cols), cols)
        normed_rows = att_buf[c].reshape(flat, chan)
        key_buf[:, here, :] = dot(normed_rows, key_weight).astype(BF16).reshape(rows, cols, chan)
        value_buf[:, here, :] = (
            dot(normed_rows, value_weight).astype(BF16).reshape(rows, cols, chan)
        )

    def att_wait(c):
        att_copy(c, {"sub": mate}, att_pass.at[0]).wait_recv()

    def ring_sent(step, carry):
        for chunk in range(CHUNKS):
            wanted = (step + 1 < last) | (chunk // half_chunks == side)

            @pl.when(wanted)
            def _():
                for part in range(subs):
                    ring_copy(step, part, chunk).wait_send()

        return carry

    def parts_sent(origin, carry):
        for h in range(2):

            @pl.when(takes(origin, h) & (origin // per_owner != g))
            def _():
                part_copy(origin, h).wait_send()

        return carry

    lax.fori_loop(0, last, ring_sent, 0)
    for chunk in range(CHUNKS):
        for way in range(2):
            first_copy(way, chunk).wait_send()
    mate_copy(right_buf.at[z, core], 0).wait_send()
    mate_copy(left_here.at[core], 1).wait_send()
    lax.fori_loop(0, planes, parts_sent, 0)

    key_value(g)
    waiting = list(by_distance)
    for d in [0] + sorted(range(1, chips), key=lambda d: min(d, chips - d)):
        if d:
            c = lax.rem(x + d, chips) * subs + core
            att_wait(c)
            att_over(d).start()
            key_value(c)
        c = lax.rem(x + d, chips) * subs + mate
        att_wait(c)
        key_value(c)
        if len(waiting) > 2:
            for m in waiting[:2]:
                pass_bias(m)
            waiting = waiting[2:]

    lane_head = lax.broadcasted_iota(jnp.int32, (cols, chan), 1) // (chan // heads)

    def raw_scores(i, carry):
        query = query_buf[pl.ds(pl.multiple_of(i * cols, cols), cols), :]
        stack = jnp.concatenate(
            [jnp.where(lane_head == h, query, jnp.zeros_like(query)) for h in range(heads)], axis=0
        )
        score_buf[i] = dot_nt(stack, key_buf[i])
        return carry

    lax.fori_loop(0, rows, raw_scores, 0, unroll=2)
    for m in waiting:
        pass_bias(m)

    for d in range(groups):
        c = lax.rem(g + d, groups)
        for p in range(per_owner):
            source = g * per_owner + p
            came = (lax.rem(source + planes - z, STRIDE) != 0) if d == 0 else c >= 0

            @pl.when(came)
            def _():
                pltpu.make_async_remote_copy(
                    src_ref=bias_z.at[0],
                    dst_ref=bias_x.at[c, p],
                    send_sem=bz_near.at[0, 0],
                    recv_sem=bx_recv.at[c, p],
                    device_id=in_plane(g),
                    device_id_type=MESH,
                ).wait_recv()

    sums = [jnp.zeros((per_owner * packed_rows, residues), F32) for _ in range(2)]
    for d in range(groups):
        c = lax.rem(g + d, groups)
        piece = bias_x[c].reshape(per_owner * packed_rows, chan)
        for q in range(2):
            spread = one_hot(
                chan, residues, lambda r, k: (k - c * cols == r - q * cols) & (r >= q * cols) & (r < (q + 1) * cols)
            )
            sums[q] = sums[q] + dot(piece, spread)
    bias = jnp.zeros((heads * cols, residues), F32)
    for q in range(2):
        def match(r, c):
            h, j = r // cols, lax.rem(r, cols)
            p, j = j // rows, lax.rem(j, rows)
            return (j // half_rows == q) & (
                c == p * packed_rows + h * half_rows + lax.rem(j, half_rows)
            )

        bias = bias + dot(
            one_hot(heads * cols, per_owner * packed_rows, match), sums[q].astype(BF16)
        )
    bias_buf[...] = bias + (residue_live - 1.0) * MASK_PENALTY

    def attend(i, carry):
        scores = score_buf[i] + bias_buf[...]
        raised = jnp.exp(scores - jnp.max(scores, axis=-1, keepdims=True))
        weights = (raised * (1.0 / jnp.sum(raised, axis=-1, keepdims=True))).astype(BF16)
        mixed = dot(weights, value_buf[i])
        attended = jnp.zeros((cols, chan), F32)
        for h in range(heads):
            attended = jnp.where(lane_head == h, mixed[h * cols : (h + 1) * cols, :], attended)
        here = pl.ds(pl.multiple_of(i * cols, cols), cols)
        gated_buf[here, :] = (attended * gate_buf[here, :]).astype(BF16)
        return carry

    lax.fori_loop(0, rows, attend, 0, unroll=2)
    out_ref[...] = (mid_buf[...] + dot(gated_buf[...], w_out_ref[...])).reshape(rows, cols, chan)

    for m in range(hops):
        if m:
            bz_far_copy(m).wait_send()
        for n in range(len(near)):

            @pl.when(leaves(m, n))
            def _():
                bz_near_copy(m, n).wait_send()

    for d in range(chips):
        if d:
            att_across(d).wait_send()
        att_over(d).wait_send()


def solution(mesh):
    planes = mesh.shape["row"]
    subs = mesh.shape["sub"]
    chips = mesh.shape["col"]
    groups = chips * subs

    def body(
        pair,
        residue_mask,
        tri_norm_gain,
        tri_in_weight,
        tri_gate_weight,
        tri_out_norm_gain,
        tri_out_weight,
        att_norm_gain,
        att_proj_weight,
        att_bias_weight,
        att_out_weight,
    ):
        rows, cols, chan = pair.shape
        heads = att_bias_weight.shape[1]
        residues = residue_mask.shape[0]
        flat = rows * cols
        per_owner = planes // groups
        packed = heads * rows // 2
        vmem = pl.BlockSpec(memory_space=pltpu.VMEM)
        dma = pltpu.SemaphoreType.DMA
        operands = (
            pair,
            residue_mask,
            tri_norm_gain[None, :],
            tri_in_weight.reshape(-1, chan),
            tri_gate_weight,
            tri_out_norm_gain[None, :],
            tri_out_weight,
            att_norm_gain[None, :],
            att_proj_weight.reshape(-1, chan),
            att_bias_weight.T,
            att_out_weight,
        )
        return pl.pallas_call(
            functools.partial(kernel, planes, chips, subs, heads),
            out_shape=jax.ShapeDtypeStruct(pair.shape, F32),
            in_specs=[vmem] * len(operands),
            out_specs=vmem,
            scratch_shapes=[
                pltpu.VMEM((planes, subs, rows, cols, chan), BF16),
                pltpu.VMEM((subs, rows, cols, chan), BF16),
                pltpu.VMEM((subs, rows, cols, chan), F32),
                pltpu.VMEM((flat, chan), BF16),
                pltpu.VMEM((4 * chan, chan), F32),
                pltpu.VMEM((rows * rows // 2, chan), F32),
                pltpu.VMEM((planes, 2, rows * rows // 2, chan), F32),
                pltpu.VMEM((chips, per_owner, 2, rows * rows // 2, chan), F32),
                pltpu.VMEM((flat, chan), F32),
                pltpu.VMEM((flat, chan), F32),
                pltpu.VMEM((groups, rows, cols, chan), BF16),
                pltpu.VMEM((rows, residues, chan), BF16),
                pltpu.VMEM((rows, residues, chan), BF16),
                pltpu.VMEM((flat, chan), BF16),
                pltpu.VMEM((flat, chan), F32),
                pltpu.VMEM((rows, heads * cols, residues), F32),
                pltpu.VMEM((flat, chan), F32),
                pltpu.VMEM((rows * 8, cols), F32),
                pltpu.VMEM((planes, packed, chan), BF16),
                pltpu.VMEM((groups, per_owner, packed, chan), BF16),
                pltpu.VMEM((heads * cols, residues), F32),
                pltpu.VMEM((flat, chan), BF16),
                dma((planes // 2, subs, CHUNKS)),
                dma((planes // 2, subs, CHUNKS)),
                dma((2, CHUNKS)),
                dma((2,)),
                dma((2,)),
                pltpu.SemaphoreType.REGULAR,
                pltpu.SemaphoreType.REGULAR,
                dma((planes, 2)),
                dma((chips, per_owner, 2)),
                dma((chips,)),
                dma((chips,)),
                dma((groups,)),
                dma((planes // STRIDE,)),
                dma((planes // STRIDE, 4)),
                dma((planes,)),
                dma((groups, per_owner)),
            ],
            compiler_params=pltpu.CompilerParams(
                collective_id=0, has_side_effects=True, vmem_limit_bytes=56 * 1024 * 1024
            ),
            name="pair_update",
        )(*operands)

    placed = (P(("parts", "row"), ("col", "sub"), None), P("parts")) + (P(),) * 9
    return jax.shard_map(
        body,
        mesh=mesh,
        in_specs=placed,
        out_specs=P(("parts", "row"), ("col", "sub"), None),
        check_vma=False,
    )
```

```python
import functools

import jax
import jax.numpy as jnp
from jax import lax
from jax.experimental import pallas as pl
from jax.experimental.pallas import tpu as pltpu
from jax.sharding import PartitionSpec as P

MESH = pl.DeviceIdType.MESH
EPSILON = 1e-05
MASK_PENALTY = 1000000000.0
F32 = jnp.float32
BF16 = jnp.bfloat16
CHUNKS = 4
STRIDE = 4
LAG = 2


def norm_last(values_in, gain):
    center = jnp.mean(values_in, axis=-1, keepdims=True)
    centered = values_in - center
    variance = jnp.mean(centered * centered, axis=-1, keepdims=True)
    return centered * lax.rsqrt(variance + EPSILON) * gain


def dot(a, b):
    return lax.dot_general(a, b, (((1,), (0,)), ((), ())), preferred_element_type=F32)


def dot_nt(a, b):
    return lax.dot_general(a, b, (((1,), (1,)), ((), ())), preferred_element_type=F32)


def one_hot(rows, cols, match):
    r = lax.broadcasted_iota(jnp.int32, (rows, cols), 0)
    c = lax.broadcasted_iota(jnp.int32, (rows, cols), 1)
    return jnp.where(match(r, c), 1.0, 0.0).astype(BF16)


def kernel(
    planes,
    chips,
    subs,
    heads,
    pair_ref,
    mask_ref,
    gain1_ref,
    w_in_ref,
    w_gate_ref,
    gain2_ref,
    w_tri_ref,
    gain3_ref,
    w_att_ref,
    w_bias_ref,
    w_out_ref,
    out_ref,
    right_buf,
    left_here,
    left_buf,
    normed_buf,
    weight_buf,
    stage_buf,
    part_buf,
    relay_buf,
    sum_buf,
    tmp_buf,
    tri_buf,
    att_buf,
    key_buf,
    value_buf,
    query_buf,
    gate_buf,
    score_buf,
    mid_buf,
    bias_rows,
    bias_z,
    bias_x,
    bias_buf,
    gated_buf,
    ring_send,
    ring_recv,
    first_send,
    mate_send,
    mate_recv,
    mate_done,
    plane_done,
    part_send,
    relay_recv,
    part_recv,
    att_send,
    att_pass,
    att_recv,
    bz_far,
    bz_near,
    bz_recv,
    bx_recv,
):
    rows, cols, chan = pair_ref.shape
    groups = chips * subs
    flat = rows * cols
    per_owner = planes // groups
    residues = groups * cols
    z = lax.axis_index("row")
    x = lax.axis_index("col")
    core = lax.axis_index("sub")
    g = x * subs + core
    mate = 1 - core
    ahead = lax.rem(z + planes + 2 * core - 1, planes)
    upper = lax.rem(z + 1, planes)
    lower = lax.rem(z + planes - 1, planes)

    def in_plane(c):
        return {"col": c // subs, "sub": lax.rem(c, subs)}

    barrier = pltpu.get_barrier_semaphore()
    for other in (upper, lower):
        for s in range(subs):
            pl.semaphore_signal(
                barrier, inc=1, device_id={"row": other, "sub": s}, device_id_type=MESH
            )
    for d in range(1, groups):
        pl.semaphore_signal(
            barrier, inc=1, device_id=in_plane(lax.rem(g + d, groups)), device_id_type=MESH
        )

    pair = pair_ref[...].reshape(flat, chan)
    normed = norm_last(pair, gain1_ref[...]).astype(BF16)
    normed_buf[...] = normed
    residue_live = mask_ref[...].reshape(1, residues).astype(F32)
    live_rows_of = jnp.broadcast_to(residue_live, (chan, residues)).astype(BF16)
    live_rows = dot_nt(one_hot(16, residues, lambda r, c: c == r + z * rows), live_rows_of)
    live_cols = dot_nt(one_hot(cols, residues, lambda r, c: c == r + g * cols), live_rows_of)
    live = jnp.concatenate([live_rows[i : i + 1] * live_cols for i in range(rows)], axis=0)
    weight_buf[...] = w_in_ref[...].astype(F32)

    def weight(p):
        return weight_buf[pl.ds(p, chan, stride=4), :].astype(BF16)

    def factor(p):
        gate = dot(normed, weight(p))
        value = dot(normed, weight(p + 1))
        return (jax.nn.sigmoid(gate) * value * live).astype(BF16)

    right_buf[z, core] = factor(2).reshape(rows, cols, chan)
    pl.semaphore_wait(barrier, 2 * subs + groups - 1)

    chunk_rows = rows // CHUNKS
    half = planes // 2
    last = half - 1

    def piece(origin, part, chunk):
        return right_buf.at[origin, part, pl.ds(chunk * chunk_rows, chunk_rows)]

    def behind(step):
        return lax.rem(z + 2 * planes - (2 * core - 1) * (1 + step), planes)

    def first_copy(way, chunk):
        return pltpu.make_async_remote_copy(
            src_ref=piece(z, core, chunk),
            dst_ref=piece(z, core, chunk),
            send_sem=first_send.at[way, chunk],
            recv_sem=ring_recv.at[0, core, chunk],
            device_id={"row": upper if way else lower, "sub": way},
            device_id_type=MESH,
        )

    def ring_copy(step, part, chunk):
        return pltpu.make_async_remote_copy(
            src_ref=piece(behind(step), part, chunk),
            dst_ref=piece(behind(step), part, chunk),
            send_sem=ring_send.at[step, part, chunk],
            recv_sem=ring_recv.at[step + 1, part, chunk],
            device_id={"row": ahead},
            device_id_type=MESH,
        )

    def ring_wait(step, part, chunk):
        block = piece(behind(step), part, chunk)
        pltpu.make_async_remote_copy(
            src_ref=block,
            dst_ref=block,
            send_sem=ring_send.at[0, part, chunk],
            recv_sem=ring_recv.at[step, part, chunk],
            device_id={"row": ahead},
            device_id_type=MESH,
        ).wait_recv()

    def mate_copy(ref, k):
        return pltpu.make_async_remote_copy(
            src_ref=ref,
            dst_ref=ref,
            send_sem=mate_send.at[k],
            recv_sem=mate_recv.at[k],
            device_id={"sub": mate},
            device_id_type=MESH,
        )

    for chunk in range(CHUNKS):
        for way in range(2):
            first_copy(way, chunk).start()
    mate_copy(right_buf.at[z, core], 0).start()
    left = factor(0)
    left_here[core] = left.reshape(rows, cols, chan)
    mate_copy(left_here.at[core], 1).start()
    left_buf[core] = left.astype(F32).reshape(rows, cols, chan)
    weight_buf[...] = w_att_ref[...].astype(F32)

    side = 1 - core
    half_chunks = CHUNKS // 2

    def products(origin, first, chunk):
        for j in range(chunk_rows):
            total = jnp.zeros((rows, chan), F32)
            for part in range(subs):
                right = right_buf[origin, part, (first + chunk) * chunk_rows + j].astype(F32)
                total = total + jnp.sum(left_buf[part] * right[None], axis=1)
            row = (chunk * chunk_rows + j) * rows
            stage_buf[row : row + rows, :] = total

    def part_copy(origin, h):
        return pltpu.make_async_remote_copy(
            src_ref=part_buf.at[origin, h],
            dst_ref=sum_buf.at[x, lax.rem(origin, per_owner), h],
            send_sem=part_send.at[origin, h],
            recv_sem=part_recv.at[x, lax.rem(origin, per_owner), h],
            device_id=in_plane(origin // per_owner),
            device_id_type=MESH,
        )

    relayed = chips == 4

    def away(origin):
        return lax.rem(x + chips - origin // per_owner // subs, chips)

    def relays(origin, h):
        return (away(origin) == 1 + 2 * h) & relayed

    def relay_copy(origin, h):
        return pltpu.make_async_remote_copy(
            src_ref=part_buf.at[origin, h],
            dst_ref=relay_buf.at[origin, h],
            send_sem=part_send.at[origin, h],
            recv_sem=relay_recv.at[origin, h],
            device_id={"col": lax.rem(x + chips + 2 * h - 1, chips)},
            device_id_type=MESH,
        )

    def to_owner(origin, h):
        mine = origin // per_owner == g
        opposite = (away(origin) == 2) & relayed

        @pl.when(mine)
        def _():
            sum_buf[x, lax.rem(origin, per_owner), h] = stage_buf[...]

        @pl.when(jnp.logical_not(mine))
        def _():
            part_buf[origin, h] = stage_buf[...]

        @pl.when(opposite)
        def _():
            relay_copy(origin, h).start()

        @pl.when(jnp.logical_not(mine | opposite | relays(origin, h)))
        def _():
            part_copy(origin, h).start()

    def relay(origin, h):
        @pl.when(relays(origin, h))
        def _():
            relay_copy(origin, h).wait_recv()
            part_buf[origin, h] = part_buf[origin, h] + relay_buf[origin, h]
            part_copy(origin, h).start()

    def takes(origin, h):
        gap = lax.rem(z + planes - origin, planes)
        shared = (gap == 0) | (gap == half)
        return (shared & (side == h)) | (jnp.logical_not(shared) & ((gap < half) == (core == 1)))

    mate_copy(right_buf.at[z, mate], 0).wait_recv()
    mate_copy(left_here.at[mate], 1).wait_recv()
    left_buf[mate] = left_here[mate].astype(F32)
    for chunk in range(half_chunks):
        products(z, side * half_chunks, chunk)
    to_owner(z, side)

    def ring_step(step, carry):
        origin = behind(step)
        for chunk in range(CHUNKS):
            wanted = (step + 1 < last) | (chunk // half_chunks == side)
            for part in range(subs):
                ring_wait(step, part, chunk)

                @pl.when(wanted)
                def _():
                    ring_copy(step, part, chunk).start()

            h = chunk // half_chunks
            products(origin, h * half_chunks, chunk % half_chunks)
            if chunk % half_chunks == half_chunks - 1:
                to_owner(origin, h)
        if relayed:

            @pl.when(step == 1)
            def _():
                relay(z, side)

            @pl.when(step >= LAG)
            def _():
                for h in range(2):
                    relay(behind(step - LAG), h)

        return carry

    lax.fori_loop(0, last, ring_step, 0)
    far = lax.rem(z + half, planes)
    for k in range(half_chunks):
        for part in range(subs):
            ring_wait(last, part, side * half_chunks + k)
        products(far, side * half_chunks, k)
    to_owner(far, side)
    if relayed:
        for step in range(last - LAG, last):
            for h in range(2):
                relay(behind(step), h)
        relay(far, side)
    pl.semaphore_signal(mate_done, inc=1, device_id={"sub": mate}, device_id_type=MESH)
    for d in range(1, groups):
        pl.semaphore_signal(
            plane_done, inc=1, device_id=in_plane(lax.rem(g + d, groups)), device_id_type=MESH
        )

    tri_gate = jax.nn.sigmoid(dot(normed_buf[...], w_gate_ref[...]))

    givers = (0, 1, 3) if relayed else tuple(range(chips))
    block = rows * rows
    for p in range(per_owner):
        origin = g * per_owner + p
        for h in range(2):
            for d in givers:
                chip = lax.rem(x + d, chips)

                @pl.when(jnp.logical_not(takes(origin, h)) if d == 0 else chip >= 0)
                def _():
                    pltpu.make_async_remote_copy(
                        src_ref=part_buf.at[0, h],
                        dst_ref=sum_buf.at[chip, p, h],
                        send_sem=part_send.at[0, h],
                        recv_sem=part_recv.at[chip, p, h],
                        device_id=in_plane(g),
                        device_id_type=MESH,
                    ).wait_recv()

            total = sum_buf[x, p, h]
            for d in givers[1:]:
                total = total + sum_buf[lax.rem(x + d, chips), p, h]
            at = p * block + h * (block // 2)
            tmp_buf[at : at + block // 2, :] = total
    for i in range(rows):
        tri_buf[i * cols : (i + 1) * cols, :] = tmp_buf[pl.ds(i, cols, stride=rows), :]

    hidden = norm_last(tri_buf[...], gain2_ref[...]).astype(BF16)
    pair_mid = pair_ref[...].reshape(flat, chan) + tri_gate * dot(hidden, w_tri_ref[...])
    mid_buf[...] = pair_mid
    att = norm_last(pair_mid, gain3_ref[...]).astype(BF16)
    att_buf[g] = att.reshape(rows, cols, chan)

    w_bias = jnp.concatenate(
        [w_bias_ref[...].astype(F32), jnp.zeros((8 - heads, chan), F32)], axis=0
    ).astype(BF16)

    for j in range(rows):
        bias_rows[j * 8 : (j + 1) * 8, :] = dot_nt(w_bias, att[j * cols : (j + 1) * cols, :])
    packed_rows = bias_z.shape[1]
    half_rows = rows // 2
    stacked = bias_rows[...].astype(BF16)
    message = jnp.zeros((packed_rows, chan), F32)
    for q in range(2):
        pick = one_hot(
            packed_rows,
            rows * 8,
            lambda r, c: c == (q * half_rows + lax.rem(r, half_rows)) * 8 + r // half_rows,
        )
        spread = one_hot(cols, chan, lambda r, c: c == r + q * cols)
        message = message + dot(dot(pick, stacked).astype(BF16), spread)
    bias_z[z] = message.astype(BF16)

    hops = planes // STRIDE
    near = (1, planes - 1, 2, 0)

    def bz_copy(source, target, sem):
        return pltpu.make_async_remote_copy(
            src_ref=bias_z.at[source],
            dst_ref=bias_z.at[source],
            send_sem=sem,
            recv_sem=bz_recv.at[source],
            device_id={"row": target},
            device_id_type=MESH,
        )

    def bz_wait(source):
        bz_copy(source, z, bz_far.at[0]).wait_recv()

    def bz_far_copy(m):
        return bz_copy(z, lax.rem(z + STRIDE * m, planes), bz_far.at[m])

    def bz_near_copy(m, n):
        source = lax.rem(z + STRIDE * m, planes)
        return pltpu.make_async_remote_copy(
            src_ref=bias_z.at[source],
            dst_ref=bias_x.at[g, lax.rem(source, per_owner)],
            send_sem=bz_near.at[m, n],
            recv_sem=bx_recv.at[g, lax.rem(source, per_owner)],
            device_id={"row": lax.rem(z + near[n], planes), **in_plane(source // per_owner)},
            device_id_type=MESH,
        )

    def leaves(m, n):
        return (lax.rem(z + STRIDE * m, planes) // per_owner != g) if near[n] == 0 else g >= 0

    by_distance = sorted(range(1, hops), key=lambda m: min(m, hops - m))

    def pass_bias(m):
        if m:
            bz_wait(lax.rem(z + STRIDE * m, planes))
        for n in range(len(near)):

            @pl.when(leaves(m, n))
            def _():
                bz_near_copy(m, n).start()

        source = lax.rem(z + STRIDE * m, planes)

        @pl.when(source // per_owner == g)
        def _():
            bias_x[g, lax.rem(source, per_owner)] = bias_z[source]

    pl.semaphore_wait(mate_done, 1)
    for m in reversed(by_distance):
        bz_far_copy(m).start()
    pl.semaphore_wait(plane_done, groups - 1)
    pass_bias(0)

    def att_copy(source, target, sem):
        return pltpu.make_async_remote_copy(
            src_ref=att_buf.at[source],
            dst_ref=att_buf.at[source],
            send_sem=sem,
            recv_sem=att_recv.at[source],
            device_id=target,
            device_id_type=MESH,
        )

    def att_across(d):
        return att_copy(g, {"col": lax.rem(x + d, chips)}, att_send.at[d])

    def att_over(d):
        return att_copy(lax.rem(x + d, chips) * subs + core, {"sub": mate}, att_pass.at[d])

    for d in sorted(range(1, chips), key=lambda d: -min(d, chips - d)):
        att_across(d).start()
    att_over(0).start()

    def att_weight(p):
        return weight_buf[pl.ds(p, chan, stride=4), :].astype(BF16)

    scale = (chan // heads) ** (-0.5)
    query_buf[...] = (dot(att, att_weight(0)) * scale).astype(BF16)
    gate_buf[...] = jax.nn.sigmoid(dot(att, att_weight(3)))
    key_weight, value_weight = att_weight(1), att_weight(2)

    def key_value(c):
        here = pl.ds(pl.multiple_of(c * cols, cols), cols)
        normed_rows = att_buf[c].reshape(flat, chan)
        key_buf[:, here, :] = dot(normed_rows, key_weight).astype(BF16).reshape(rows, cols, chan)
        value_buf[:, here, :] = (
            dot(normed_rows, value_weight).astype(BF16).reshape(rows, cols, chan)
        )

    def att_wait(c):
        att_copy(c, {"sub": mate}, att_pass.at[0]).wait_recv()

    def ring_sent(step, carry):
        for chunk in range(CHUNKS):
            wanted = (step + 1 < last) | (chunk // half_chunks == side)

            @pl.when(wanted)
            def _():
                for part in range(subs):
                    ring_copy(step, part, chunk).wait_send()

        return carry

    def parts_sent(origin, carry):
        for h in range(2):

            @pl.when(takes(origin, h) & (origin // per_owner != g))
            def _():
                part_copy(origin, h).wait_send()

        return carry

    lax.fori_loop(0, last, ring_sent, 0)
    for chunk in range(CHUNKS):
        for way in range(2):
            first_copy(way, chunk).wait_send()
    mate_copy(right_buf.at[z, core], 0).wait_send()
    mate_copy(left_here.at[core], 1).wait_send()
    lax.fori_loop(0, planes, parts_sent, 0)

    key_value(g)
    waiting = list(by_distance)
    for d in [0] + sorted(range(1, chips), key=lambda d: min(d, chips - d)):
        if d:
            c = lax.rem(x + d, chips) * subs + core
            att_wait(c)
            att_over(d).start()
            key_value(c)
        c = lax.rem(x + d, chips) * subs + mate
        att_wait(c)
        key_value(c)
        if len(waiting) > 2:
            for m in waiting[:2]:
                pass_bias(m)
            waiting = waiting[2:]

    lane_head = lax.broadcasted_iota(jnp.int32, (cols, chan), 1) // (chan // heads)

    def raw_scores(i, carry):
        query = query_buf[pl.ds(pl.multiple_of(i * cols, cols), cols), :]
        stack = jnp.concatenate(
            [jnp.where(lane_head == h, query, jnp.zeros_like(query)) for h in range(heads)], axis=0
        )
        score_buf[i] = dot_nt(stack, key_buf[i])
        return carry

    lax.fori_loop(0, rows, raw_scores, 0, unroll=2)
    for m in waiting:
        pass_bias(m)

    for d in range(groups):
        c = lax.rem(g + d, groups)
        for p in range(per_owner):
            source = g * per_owner + p
            came = (lax.rem(source + planes - z, STRIDE) != 0) if d == 0 else c >= 0

            @pl.when(came)
            def _():
                pltpu.make_async_remote_copy(
                    src_ref=bias_z.at[0],
                    dst_ref=bias_x.at[c, p],
                    send_sem=bz_near.at[0, 0],
                    recv_sem=bx_recv.at[c, p],
                    device_id=in_plane(g),
                    device_id_type=MESH,
                ).wait_recv()

    sums = [jnp.zeros((per_owner * packed_rows, residues), F32) for _ in range(2)]
    for d in range(groups):
        c = lax.rem(g + d, groups)
        piece = bias_x[c].reshape(per_owner * packed_rows, chan)
        for q in range(2):
            spread = one_hot(
                chan, residues, lambda r, k: (k - c * cols == r - q * cols) & (r >= q * cols) & (r < (q + 1) * cols)
            )
            sums[q] = sums[q] + dot(piece, spread)
    bias = jnp.zeros((heads * cols, residues), F32)
    for q in range(2):
        def match(r, c):
            h, j = r // cols, lax.rem(r, cols)
            p, j = j // rows, lax.rem(j, rows)
            return (j // half_rows == q) & (
                c == p * packed_rows + h * half_rows + lax.rem(j, half_rows)
            )

        bias = bias + dot(
            one_hot(heads * cols, per_owner * packed_rows, match), sums[q].astype(BF16)
        )
    bias_buf[...] = bias + (residue_live - 1.0) * MASK_PENALTY

    def attend(i, carry):
        scores = score_buf[i] + bias_buf[...]
        raised = jnp.exp(scores - jnp.max(scores, axis=-1, keepdims=True))
        weights = (raised * (1.0 / jnp.sum(raised, axis=-1, keepdims=True))).astype(BF16)
        mixed = dot(weights, value_buf[i])
        attended = jnp.zeros((cols, chan), F32)
        for h in range(heads):
            attended = jnp.where(lane_head == h, mixed[h * cols : (h + 1) * cols, :], attended)
        here = pl.ds(pl.multiple_of(i * cols, cols), cols)
        gated_buf[here, :] = (attended * gate_buf[here, :]).astype(BF16)
        return carry

    lax.fori_loop(0, rows, attend, 0, unroll=2)
    out_ref[...] = (mid_buf[...] + dot(gated_buf[...], w_out_ref[...])).reshape(rows, cols, chan)

    for m in range(hops):
        if m:
            bz_far_copy(m).wait_send()
        for n in range(len(near)):

            @pl.when(leaves(m, n))
            def _():
                bz_near_copy(m, n).wait_send()

    for d in range(chips):
        if d:
            att_across(d).wait_send()
        att_over(d).wait_send()


def solution(mesh):
    planes = mesh.shape["row"]
    subs = mesh.shape["sub"]
    chips = mesh.shape["col"]
    groups = chips * subs

    def body(
        pair,
        residue_mask,
        tri_norm_gain,
        tri_in_weight,
        tri_gate_weight,
        tri_out_norm_gain,
        tri_out_weight,
        att_norm_gain,
        att_proj_weight,
        att_bias_weight,
        att_out_weight,
    ):
        rows, cols, chan = pair.shape
        heads = att_bias_weight.shape[1]
        residues = residue_mask.shape[0]
        flat = rows * cols
        per_owner = planes // groups
        packed = heads * rows // 2
        vmem = pl.BlockSpec(memory_space=pltpu.VMEM)
        dma = pltpu.SemaphoreType.DMA
        operands = (
            pair,
            residue_mask,
            tri_norm_gain[None, :],
            tri_in_weight.reshape(-1, chan),
            tri_gate_weight,
            tri_out_norm_gain[None, :],
            tri_out_weight,
            att_norm_gain[None, :],
            att_proj_weight.reshape(-1, chan),
            att_bias_weight.T,
            att_out_weight,
        )
        return pl.pallas_call(
            functools.partial(kernel, planes, chips, subs, heads),
            out_shape=jax.ShapeDtypeStruct(pair.shape, F32),
            in_specs=[vmem] * len(operands),
            out_specs=vmem,
            scratch_shapes=[
                pltpu.VMEM((planes, subs, rows, cols, chan), BF16),
                pltpu.VMEM((subs, rows, cols, chan), BF16),
                pltpu.VMEM((subs, rows, cols, chan), F32),
                pltpu.VMEM((flat, chan), BF16),
                pltpu.VMEM((4 * chan, chan), F32),
                pltpu.VMEM((rows * rows // 2, chan), F32),
                pltpu.VMEM((planes, 2, rows * rows // 2, chan), F32),
                pltpu.VMEM((planes, 2, rows * rows // 2, chan), F32),
                pltpu.VMEM((chips, per_owner, 2, rows * rows // 2, chan), F32),
                pltpu.VMEM((flat, chan), F32),
                pltpu.VMEM((flat, chan), F32),
                pltpu.VMEM((groups, rows, cols, chan), BF16),
                pltpu.VMEM((rows, residues, chan), BF16),
                pltpu.VMEM((rows, residues, chan), BF16),
                pltpu.VMEM((flat, chan), BF16),
                pltpu.VMEM((flat, chan), F32),
                pltpu.VMEM((rows, heads * cols, residues), F32),
                pltpu.VMEM((flat, chan), F32),
                pltpu.VMEM((rows * 8, cols), F32),
                pltpu.VMEM((planes, packed, chan), BF16),
                pltpu.VMEM((groups, per_owner, packed, chan), BF16),
                pltpu.VMEM((heads * cols, residues), F32),
                pltpu.VMEM((flat, chan), BF16),
                dma((planes // 2, subs, CHUNKS)),
                dma((planes // 2, subs, CHUNKS)),
                dma((2, CHUNKS)),
                dma((2,)),
                dma((2,)),
                pltpu.SemaphoreType.REGULAR,
                pltpu.SemaphoreType.REGULAR,
                dma((planes, 2)),
                dma((planes, 2)),
                dma((chips, per_owner, 2)),
                dma((chips,)),
                dma((chips,)),
                dma((groups,)),
                dma((planes // STRIDE,)),
                dma((planes // STRIDE, 4)),
                dma((planes,)),
                dma((groups, per_owner)),
            ],
            compiler_params=pltpu.CompilerParams(
                collective_id=0, has_side_effects=True, vmem_limit_bytes=56 * 1024 * 1024
            ),
            name="pair_update",
        )(*operands)

    placed = (P(("parts", "row"), ("col", "sub"), None), P("parts")) + (P(),) * 9
    return jax.shard_map(
        body,
        mesh=mesh,
        in_specs=placed,
        out_specs=P(("parts", "row"), ("col", "sub"), None),
        check_vma=False,
    )
```

```python
import functools

import jax
import jax.numpy as jnp
from jax import lax
from jax.experimental import pallas as pl
from jax.experimental.pallas import tpu as pltpu
from jax.sharding import PartitionSpec as P

MESH = pl.DeviceIdType.MESH
EPSILON = 1e-05
MASK_PENALTY = 1000000000.0
F32 = jnp.float32
BF16 = jnp.bfloat16
CHUNKS = 4
STRIDE = 4


def norm_last(values_in, gain):
    center = jnp.mean(values_in, axis=-1, keepdims=True)
    centered = values_in - center
    variance = jnp.mean(centered * centered, axis=-1, keepdims=True)
    return centered * lax.rsqrt(variance + EPSILON) * gain


def dot(a, b):
    return lax.dot_general(a, b, (((1,), (0,)), ((), ())), preferred_element_type=F32)


def dot_nt(a, b):
    return lax.dot_general(a, b, (((1,), (1,)), ((), ())), preferred_element_type=F32)


def one_hot(rows, cols, match):
    r = lax.broadcasted_iota(jnp.int32, (rows, cols), 0)
    c = lax.broadcasted_iota(jnp.int32, (rows, cols), 1)
    return jnp.where(match(r, c), 1.0, 0.0).astype(BF16)


def kernel(
    planes,
    chips,
    subs,
    heads,
    pair_ref,
    mask_ref,
    gain1_ref,
    w_in_ref,
    w_gate_ref,
    gain2_ref,
    w_tri_ref,
    gain3_ref,
    w_att_ref,
    w_bias_ref,
    w_out_ref,
    out_ref,
    right_buf,
    left_here,
    left_buf,
    normed_buf,
    weight_buf,
    stage_buf,
    part_buf,
    sum_buf,
    tmp_buf,
    tri_buf,
    att_buf,
    key_buf,
    value_buf,
    query_buf,
    gate_buf,
    score_buf,
    mid_buf,
    bias_rows,
    bias_z,
    bias_x,
    bias_buf,
    gated_buf,
    ring_send,
    ring_recv,
    first_send,
    mate_send,
    mate_recv,
    mate_done,
    plane_done,
    part_send,
    part_recv,
    att_send,
    att_pass,
    att_recv,
    bz_far,
    bz_near,
    bz_recv,
    bx_recv,
):
    rows, cols, chan = pair_ref.shape
    groups = chips * subs
    flat = rows * cols
    per_owner = planes // groups
    residues = groups * cols
    z = lax.axis_index("row")
    x = lax.axis_index("col")
    core = lax.axis_index("sub")
    g = x * subs + core
    mate = 1 - core
    ahead = lax.rem(z + planes + 2 * core - 1, planes)
    upper = lax.rem(z + 1, planes)
    lower = lax.rem(z + planes - 1, planes)

    def in_plane(c):
        return {"col": c // subs, "sub": lax.rem(c, subs)}

    barrier = pltpu.get_barrier_semaphore()
    for other in (upper, lower):
        for s in range(subs):
            pl.semaphore_signal(
                barrier, inc=1, device_id={"row": other, "sub": s}, device_id_type=MESH
            )
    for d in range(1, groups):
        pl.semaphore_signal(
            barrier, inc=1, device_id=in_plane(lax.rem(g + d, groups)), device_id_type=MESH
        )

    pair = pair_ref[...].reshape(flat, chan)
    normed = norm_last(pair, gain1_ref[...]).astype(BF16)
    normed_buf[...] = normed
    residue_live = mask_ref[...].reshape(1, residues).astype(F32)
    live_rows_of = jnp.broadcast_to(residue_live, (chan, residues)).astype(BF16)
    live_rows = dot_nt(one_hot(16, residues, lambda r, c: c == r + z * rows), live_rows_of)
    live_cols = dot_nt(one_hot(cols, residues, lambda r, c: c == r + g * cols), live_rows_of)
    live = jnp.concatenate([live_rows[i : i + 1] * live_cols for i in range(rows)], axis=0)
    weight_buf[...] = w_in_ref[...].astype(F32)

    def weight(p):
        return weight_buf[pl.ds(p, chan, stride=4), :].astype(BF16)

    def factor(p):
        gate = dot(normed, weight(p))
        value = dot(normed, weight(p + 1))
        return (jax.nn.sigmoid(gate) * value * live).astype(BF16)

    right_buf[z, core] = factor(2).reshape(rows, cols, chan)
    pl.semaphore_wait(barrier, 2 * subs + groups - 1)

    chunk_rows = rows // CHUNKS
    half = planes // 2
    last = half - 1

    def piece(origin, part, chunk):
        return right_buf.at[origin, part, pl.ds(chunk * chunk_rows, chunk_rows)]

    def behind(step):
        return lax.rem(z + 2 * planes - (2 * core - 1) * (1 + step), planes)

    def first_copy(way, chunk):
        return pltpu.make_async_remote_copy(
            src_ref=piece(z, core, chunk),
            dst_ref=piece(z, core, chunk),
            send_sem=first_send.at[way, chunk],
            recv_sem=ring_recv.at[0, core, chunk],
            device_id={"row": upper if way else lower, "sub": way},
            device_id_type=MESH,
        )

    def ring_copy(step, part, chunk):
        return pltpu.make_async_remote_copy(
            src_ref=piece(behind(step), part, chunk),
            dst_ref=piece(behind(step), part, chunk),
            send_sem=ring_send.at[step, part, chunk],
            recv_sem=ring_recv.at[step + 1, part, chunk],
            device_id={"row": ahead},
            device_id_type=MESH,
        )

    def ring_wait(step, part, chunk):
        block = piece(behind(step), part, chunk)
        pltpu.make_async_remote_copy(
            src_ref=block,
            dst_ref=block,
            send_sem=ring_send.at[0, part, chunk],
            recv_sem=ring_recv.at[step, part, chunk],
            device_id={"row": ahead},
            device_id_type=MESH,
        ).wait_recv()

    def mate_copy(ref, k):
        return pltpu.make_async_remote_copy(
            src_ref=ref,
            dst_ref=ref,
            send_sem=mate_send.at[k],
            recv_sem=mate_recv.at[k],
            device_id={"sub": mate},
            device_id_type=MESH,
        )

    for chunk in range(CHUNKS):
        for way in range(2):
            first_copy(way, chunk).start()
    mate_copy(right_buf.at[z, core], 0).start()
    left = factor(0)
    left_here[core] = left.reshape(rows, cols, chan)
    mate_copy(left_here.at[core], 1).start()
    left_buf[core] = left.astype(F32).reshape(rows, cols, chan)
    weight_buf[...] = w_att_ref[...].astype(F32)

    side = 1 - core
    half_chunks = CHUNKS // 2

    def products(origin, first, chunk):
        for j in range(chunk_rows):
            total = jnp.zeros((rows, chan), F32)
            for part in range(subs):
                right = right_buf[origin, part, (first + chunk) * chunk_rows + j].astype(F32)
                total = total + jnp.sum(left_buf[part] * right[None], axis=1)
            row = (chunk * chunk_rows + j) * rows
            stage_buf[row : row + rows, :] = total

    def part_copy(origin, h):
        return pltpu.make_async_remote_copy(
            src_ref=part_buf.at[origin, h],
            dst_ref=sum_buf.at[x, lax.rem(origin, per_owner), h],
            send_sem=part_send.at[origin, h],
            recv_sem=part_recv.at[x, lax.rem(origin, per_owner), h],
            device_id=in_plane(origin // per_owner),
            device_id_type=MESH,
        )

    def to_owner(origin, h):
        mine = origin // per_owner == g

        @pl.when(jnp.logical_not(mine))
        def _():
            part_buf[origin, h] = stage_buf[...]
            part_copy(origin, h).start()

        @pl.when(mine)
        def _():
            sum_buf[x, lax.rem(origin, per_owner), h] = stage_buf[...]

    def takes(origin, h):
        gap = lax.rem(z + planes - origin, planes)
        shared = (gap == 0) | (gap == half)
        return (shared & (side == h)) | (jnp.logical_not(shared) & ((gap < half) == (core == 1)))

    mate_copy(right_buf.at[z, mate], 0).wait_recv()
    mate_copy(left_here.at[mate], 1).wait_recv()
    left_buf[mate] = left_here[mate].astype(F32)
    for chunk in range(half_chunks):
        products(z, side * half_chunks, chunk)
    to_owner(z, side)

    def ring_step(step, carry):
        origin = behind(step)
        for chunk in range(CHUNKS):
            wanted = (step + 1 < last) | (chunk // half_chunks == side)
            for part in range(subs):
                ring_wait(step, part, chunk)

                @pl.when(wanted)
                def _():
                    ring_copy(step, part, chunk).start()

            h = chunk // half_chunks
            products(origin, h * half_chunks, chunk % half_chunks)
            if chunk % half_chunks == half_chunks - 1:
                to_owner(origin, h)
        return carry

    lax.fori_loop(0, last, ring_step, 0)
    far = lax.rem(z + half, planes)
    for k in range(half_chunks):
        for part in range(subs):
            ring_wait(last, part, side * half_chunks + k)
        products(far, side * half_chunks, k)
    to_owner(far, side)
    pl.semaphore_signal(mate_done, inc=1, device_id={"sub": mate}, device_id_type=MESH)
    for d in range(1, groups):
        pl.semaphore_signal(
            plane_done, inc=1, device_id=in_plane(lax.rem(g + d, groups)), device_id_type=MESH
        )

    tri_gate = jax.nn.sigmoid(dot(normed_buf[...], w_gate_ref[...]))

    block = rows * rows
    for p in range(per_owner):
        origin = g * per_owner + p
        for h in range(2):
            for d in range(chips):
                chip = lax.rem(x + d, chips)

                @pl.when(jnp.logical_not(takes(origin, h)) if d == 0 else chip >= 0)
                def _():
                    pltpu.make_async_remote_copy(
                        src_ref=part_buf.at[0, h],
                        dst_ref=sum_buf.at[chip, p, h],
                        send_sem=part_send.at[0, h],
                        recv_sem=part_recv.at[chip, p, h],
                        device_id=in_plane(g),
                        device_id_type=MESH,
                    ).wait_recv()

            total = sum_buf[0, p, h]
            for chip in range(1, chips):
                total = total + sum_buf[chip, p, h]
            at = p * block + h * (block // 2)
            tmp_buf[at : at + block // 2, :] = total
    for i in range(rows):
        tri_buf[i * cols : (i + 1) * cols, :] = tmp_buf[pl.ds(i, cols, stride=rows), :]

    hidden = norm_last(tri_buf[...], gain2_ref[...]).astype(BF16)
    pair_mid = pair_ref[...].reshape(flat, chan) + tri_gate * dot(hidden, w_tri_ref[...])
    mid_buf[...] = pair_mid
    att = norm_last(pair_mid, gain3_ref[...]).astype(BF16)
    att_buf[g] = att.reshape(rows, cols, chan)

    w_bias = jnp.concatenate(
        [w_bias_ref[...].astype(F32), jnp.zeros((8 - heads, chan), F32)], axis=0
    ).astype(BF16)

    for j in range(rows):
        bias_rows[j * 8 : (j + 1) * 8, :] = dot_nt(w_bias, att[j * cols : (j + 1) * cols, :])
    packed_rows = bias_z.shape[1]
    half_rows = rows // 2
    stacked = bias_rows[...].astype(BF16)
    message = jnp.zeros((packed_rows, chan), F32)
    for q in range(2):
        pick = one_hot(
            packed_rows,
            rows * 8,
            lambda r, c: c == (q * half_rows + lax.rem(r, half_rows)) * 8 + r // half_rows,
        )
        spread = one_hot(cols, chan, lambda r, c: c == r + q * cols)
        message = message + dot(dot(pick, stacked).astype(BF16), spread)
    bias_z[z] = message.astype(BF16)

    hops = planes // STRIDE
    near = (1, planes - 1, 2, 0)

    def bz_copy(source, target, sem):
        return pltpu.make_async_remote_copy(
            src_ref=bias_z.at[source],
            dst_ref=bias_z.at[source],
            send_sem=sem,
            recv_sem=bz_recv.at[source],
            device_id={"row": target},
            device_id_type=MESH,
        )

    def bz_wait(source):
        bz_copy(source, z, bz_far.at[0]).wait_recv()

    def bz_far_copy(m):
        return bz_copy(z, lax.rem(z + STRIDE * m, planes), bz_far.at[m])

    def bz_near_copy(m, n):
        source = lax.rem(z + STRIDE * m, planes)
        return pltpu.make_async_remote_copy(
            src_ref=bias_z.at[source],
            dst_ref=bias_x.at[g, lax.rem(source, per_owner)],
            send_sem=bz_near.at[m, n],
            recv_sem=bx_recv.at[g, lax.rem(source, per_owner)],
            device_id={"row": lax.rem(z + near[n], planes), **in_plane(source // per_owner)},
            device_id_type=MESH,
        )

    def leaves(m, n):
        return (lax.rem(z + STRIDE * m, planes) // per_owner != g) if near[n] == 0 else g >= 0

    by_distance = sorted(range(1, hops), key=lambda m: min(m, hops - m))

    def pass_bias(m):
        for n in range(len(near)):

            @pl.when(leaves(m, n))
            def _():
                bz_near_copy(m, n).start()

        source = lax.rem(z + STRIDE * m, planes)

        @pl.when(source // per_owner == g)
        def _():
            bias_x[g, lax.rem(source, per_owner)] = bias_z[source]

    pl.semaphore_wait(mate_done, 1)
    for m in reversed(by_distance):
        bz_far_copy(m).start()

    def att_copy(source, target, sem):
        return pltpu.make_async_remote_copy(
            src_ref=att_buf.at[source],
            dst_ref=att_buf.at[source],
            send_sem=sem,
            recv_sem=att_recv.at[source],
            device_id=target,
            device_id_type=MESH,
        )

    def att_across(d):
        return att_copy(g, {"col": lax.rem(x + d, chips)}, att_send.at[d])

    def att_over(c):
        return att_copy(c, {"sub": mate}, att_pass.at[c // subs])

    for d in sorted(range(1, chips), key=lambda d: -min(d, chips - d)):
        att_across(d).start()
    att_over(g).start()

    def att_weight(p):
        return weight_buf[pl.ds(p, chan, stride=4), :].astype(BF16)

    scale = (chan // heads) ** (-0.5)
    query_buf[...] = (dot(att, att_weight(0)) * scale).astype(BF16)
    gate_buf[...] = jax.nn.sigmoid(dot(att, att_weight(3)))
    key_weight, value_weight = att_weight(1), att_weight(2)

    def key_value(c):
        here = pl.ds(pl.multiple_of(c * cols, cols), cols)
        normed_rows = att_buf[c].reshape(flat, chan)
        key_buf[:, here, :] = dot(normed_rows, key_weight).astype(BF16).reshape(rows, cols, chan)
        value_buf[:, here, :] = (
            dot(normed_rows, value_weight).astype(BF16).reshape(rows, cols, chan)
        )

    def att_wait(c):
        att_copy(c, {"sub": mate}, att_pass.at[0]).wait_recv()

    def ring_sent(step, carry):
        for chunk in range(CHUNKS):
            wanted = (step + 1 < last) | (chunk // half_chunks == side)

            @pl.when(wanted)
            def _():
                for part in range(subs):
                    ring_copy(step, part, chunk).wait_send()

        return carry

    def parts_sent(origin, carry):
        for h in range(2):

            @pl.when(takes(origin, h) & (origin // per_owner != g))
            def _():
                part_copy(origin, h).wait_send()

        return carry

    lax.fori_loop(0, last, ring_sent, 0)
    for chunk in range(CHUNKS):
        for way in range(2):
            first_copy(way, chunk).wait_send()
    mate_copy(right_buf.at[z, core], 0).wait_send()
    mate_copy(left_here.at[core], 1).wait_send()
    lax.fori_loop(0, planes, parts_sent, 0)

    pl.semaphore_wait(plane_done, groups - 1)
    pass_bias(0)

    late = lax.rem(z + half, planes) // per_owner

    def take_rows(k, carry):
        c = lax.rem(late + k, groups)

        @pl.when(c != g)
        def _():
            att_wait(c)

        @pl.when((c != g) & (lax.rem(c, subs) == core))
        def _():
            att_over(c).start()

        key_value(c)
        return carry

    def take_bias(k, carry):
        m = lax.rem(g + k + 2 * hops - z // STRIDE - hops // 2, hops)

        @pl.when(m != 0)
        def _():
            bz_wait(lax.rem(z + STRIDE * m, planes))
            pass_bias(m)

        return carry

    lax.fori_loop(1, groups, take_rows, 0)
    lax.fori_loop(1, hops, take_bias, 0)
    take_rows(groups, 0)

    lane_head = lax.broadcasted_iota(jnp.int32, (cols, chan), 1) // (chan // heads)

    def raw_scores(i, carry):
        query = query_buf[pl.ds(pl.multiple_of(i * cols, cols), cols), :]
        stack = jnp.concatenate(
            [jnp.where(lane_head == h, query, jnp.zeros_like(query)) for h in range(heads)], axis=0
        )
        score_buf[i] = dot_nt(stack, key_buf[i])
        return carry

    lax.fori_loop(0, rows, raw_scores, 0, unroll=2)
    take_bias(0, 0)

    for d in range(groups):
        c = lax.rem(g + d, groups)
        for p in range(per_owner):
            source = g * per_owner + p
            came = (lax.rem(source + planes - z, STRIDE) != 0) if d == 0 else c >= 0

            @pl.when(came)
            def _():
                pltpu.make_async_remote_copy(
                    src_ref=bias_z.at[0],
                    dst_ref=bias_x.at[c, p],
                    send_sem=bz_near.at[0, 0],
                    recv_sem=bx_recv.at[c, p],
                    device_id=in_plane(g),
                    device_id_type=MESH,
                ).wait_recv()

    sums = [jnp.zeros((per_owner * packed_rows, residues), F32) for _ in range(2)]
    for d in range(groups):
        c = lax.rem(g + d, groups)
        piece = bias_x[c].reshape(per_owner * packed_rows, chan)
        for q in range(2):
            spread = one_hot(
                chan, residues, lambda r, k: (k - c * cols == r - q * cols) & (r >= q * cols) & (r < (q + 1) * cols)
            )
            sums[q] = sums[q] + dot(piece, spread)
    bias = jnp.zeros((heads * cols, residues), F32)
    for q in range(2):
        def match(r, c):
            h, j = r // cols, lax.rem(r, cols)
            p, j = j // rows, lax.rem(j, rows)
            return (j // half_rows == q) & (
                c == p * packed_rows + h * half_rows + lax.rem(j, half_rows)
            )

        bias = bias + dot(
            one_hot(heads * cols, per_owner * packed_rows, match), sums[q].astype(BF16)
        )
    bias_buf[...] = bias + (residue_live - 1.0) * MASK_PENALTY

    def attend(i, carry):
        scores = score_buf[i] + bias_buf[...]
        raised = jnp.exp(scores - jnp.max(scores, axis=-1, keepdims=True))
        weights = (raised * (1.0 / jnp.sum(raised, axis=-1, keepdims=True))).astype(BF16)
        mixed = dot(weights, value_buf[i])
        attended = jnp.zeros((cols, chan), F32)
        for h in range(heads):
            attended = jnp.where(lane_head == h, mixed[h * cols : (h + 1) * cols, :], attended)
        here = pl.ds(pl.multiple_of(i * cols, cols), cols)
        gated_buf[here, :] = (attended * gate_buf[here, :]).astype(BF16)
        return carry

    lax.fori_loop(0, rows, attend, 0, unroll=2)
    out_ref[...] = (mid_buf[...] + dot(gated_buf[...], w_out_ref[...])).reshape(rows, cols, chan)

    for m in range(hops):
        if m:
            bz_far_copy(m).wait_send()
        for n in range(len(near)):

            @pl.when(leaves(m, n))
            def _():
                bz_near_copy(m, n).wait_send()

    for d in range(chips):
        if d:
            att_across(d).wait_send()
        att_over(d * subs + core).wait_send()


def solution(mesh):
    planes = mesh.shape["row"]
    subs = mesh.shape["sub"]
    chips = mesh.shape["col"]
    groups = chips * subs

    def body(
        pair,
        residue_mask,
        tri_norm_gain,
        tri_in_weight,
        tri_gate_weight,
        tri_out_norm_gain,
        tri_out_weight,
        att_norm_gain,
        att_proj_weight,
        att_bias_weight,
        att_out_weight,
    ):
        rows, cols, chan = pair.shape
        heads = att_bias_weight.shape[1]
        residues = residue_mask.shape[0]
        flat = rows * cols
        per_owner = planes // groups
        packed = heads * rows // 2
        vmem = pl.BlockSpec(memory_space=pltpu.VMEM)
        dma = pltpu.SemaphoreType.DMA
        operands = (
            pair,
            residue_mask,
            tri_norm_gain[None, :],
            tri_in_weight.reshape(-1, chan),
            tri_gate_weight,
            tri_out_norm_gain[None, :],
            tri_out_weight,
            att_norm_gain[None, :],
            att_proj_weight.reshape(-1, chan),
            att_bias_weight.T,
            att_out_weight,
        )
        return pl.pallas_call(
            functools.partial(kernel, planes, chips, subs, heads),
            out_shape=jax.ShapeDtypeStruct(pair.shape, F32),
            in_specs=[vmem] * len(operands),
            out_specs=vmem,
            scratch_shapes=[
                pltpu.VMEM((planes, subs, rows, cols, chan), BF16),
                pltpu.VMEM((subs, rows, cols, chan), BF16),
                pltpu.VMEM((subs, rows, cols, chan), F32),
                pltpu.VMEM((flat, chan), BF16),
                pltpu.VMEM((4 * chan, chan), F32),
                pltpu.VMEM((rows * rows // 2, chan), F32),
                pltpu.VMEM((planes, 2, rows * rows // 2, chan), F32),
                pltpu.VMEM((chips, per_owner, 2, rows * rows // 2, chan), F32),
                pltpu.VMEM((flat, chan), F32),
                pltpu.VMEM((flat, chan), F32),
                pltpu.VMEM((groups, rows, cols, chan), BF16),
                pltpu.VMEM((rows, residues, chan), BF16),
                pltpu.VMEM((rows, residues, chan), BF16),
                pltpu.VMEM((flat, chan), BF16),
                pltpu.VMEM((flat, chan), F32),
                pltpu.VMEM((rows, heads * cols, residues), F32),
                pltpu.VMEM((flat, chan), F32),
                pltpu.VMEM((rows * 8, cols), F32),
                pltpu.VMEM((planes, packed, chan), BF16),
                pltpu.VMEM((groups, per_owner, packed, chan), BF16),
                pltpu.VMEM((heads * cols, residues), F32),
                pltpu.VMEM((flat, chan), BF16),
                dma((planes // 2, subs, CHUNKS)),
                dma((planes // 2, subs, CHUNKS)),
                dma((2, CHUNKS)),
                dma((2,)),
                dma((2,)),
                pltpu.SemaphoreType.REGULAR,
                pltpu.SemaphoreType.REGULAR,
                dma((planes, 2)),
                dma((chips, per_owner, 2)),
                dma((chips,)),
                dma((chips,)),
                dma((groups,)),
                dma((planes // STRIDE,)),
                dma((planes // STRIDE, 4)),
                dma((planes,)),
                dma((groups, per_owner)),
            ],
            compiler_params=pltpu.CompilerParams(
                collective_id=0, has_side_effects=True, vmem_limit_bytes=56 * 1024 * 1024
            ),
            name="pair_update",
        )(*operands)

    placed = (P(("parts", "row"), ("col", "sub"), None), P("parts")) + (P(),) * 9
    return jax.shard_map(
        body,
        mesh=mesh,
        in_specs=placed,
        out_specs=P(("parts", "row"), ("col", "sub"), None),
        check_vma=False,
    )
```

```python
import functools

import jax
import jax.numpy as jnp
from jax import lax
from jax.experimental import pallas as pl
from jax.experimental.pallas import tpu as pltpu
from jax.sharding import PartitionSpec as P

MESH = pl.DeviceIdType.MESH
EPSILON = 1e-05
MASK_PENALTY = 1000000000.0
F32 = jnp.float32
BF16 = jnp.bfloat16
CHUNKS = 4
STRIDE = 4


def norm_last(values_in, gain):
    center = jnp.mean(values_in, axis=-1, keepdims=True)
    centered = values_in - center
    variance = jnp.mean(centered * centered, axis=-1, keepdims=True)
    return centered * lax.rsqrt(variance + EPSILON) * gain


def dot(a, b):
    return lax.dot_general(a, b, (((1,), (0,)), ((), ())), preferred_element_type=F32)


def dot_nt(a, b):
    return lax.dot_general(a, b, (((1,), (1,)), ((), ())), preferred_element_type=F32)


def one_hot(rows, cols, match):
    r = lax.broadcasted_iota(jnp.int32, (rows, cols), 0)
    c = lax.broadcasted_iota(jnp.int32, (rows, cols), 1)
    return jnp.where(match(r, c), 1.0, 0.0).astype(BF16)


def kernel(
    planes,
    chips,
    subs,
    heads,
    pair_ref,
    mask_ref,
    gain1_ref,
    w_in_ref,
    w_gate_ref,
    gain2_ref,
    w_tri_ref,
    gain3_ref,
    w_att_ref,
    w_bias_ref,
    w_out_ref,
    out_ref,
    right_buf,
    left_here,
    left_buf,
    normed_buf,
    weight_buf,
    stage_buf,
    part_buf,
    sum_buf,
    tmp_buf,
    tri_buf,
    att_buf,
    key_buf,
    value_buf,
    query_buf,
    gate_buf,
    score_buf,
    mid_buf,
    bias_rows,
    bias_z,
    bias_x,
    bias_buf,
    gated_buf,
    ring_send,
    ring_recv,
    first_send,
    mate_send,
    mate_recv,
    mate_done,
    plane_done,
    part_send,
    part_recv,
    att_send,
    att_pass,
    att_recv,
    bz_far,
    bz_near,
    bz_recv,
    bx_recv,
):
    rows, cols, chan = pair_ref.shape
    groups = chips * subs
    flat = rows * cols
    per_owner = planes // groups
    residues = groups * cols
    z = lax.axis_index("row")
    x = lax.axis_index("col")
    core = lax.axis_index("sub")
    g = x * subs + core
    mate = 1 - core
    ahead = lax.rem(z + planes + 2 * core - 1, planes)
    upper = lax.rem(z + 1, planes)
    lower = lax.rem(z + planes - 1, planes)

    def in_plane(c):
        return {"col": c // subs, "sub": lax.rem(c, subs)}

    barrier = pltpu.get_barrier_semaphore()
    for other in (upper, lower):
        for s in range(subs):
            pl.semaphore_signal(
                barrier, inc=1, device_id={"row": other, "sub": s}, device_id_type=MESH
            )
    for d in range(1, groups):
        pl.semaphore_signal(
            barrier, inc=1, device_id=in_plane(lax.rem(g + d, groups)), device_id_type=MESH
        )

    pair = pair_ref[...].reshape(flat, chan)
    normed = norm_last(pair, gain1_ref[...]).astype(BF16)
    normed_buf[...] = normed
    residue_live = mask_ref[...].reshape(1, residues).astype(F32)
    live_rows_of = jnp.broadcast_to(residue_live, (chan, residues)).astype(BF16)
    live_rows = dot_nt(one_hot(16, residues, lambda r, c: c == r + z * rows), live_rows_of)
    live_cols = dot_nt(one_hot(cols, residues, lambda r, c: c == r + g * cols), live_rows_of)
    live = jnp.concatenate([live_rows[i : i + 1] * live_cols for i in range(rows)], axis=0)
    weight_buf[...] = w_in_ref[...].astype(F32)

    def weight(p):
        return weight_buf[pl.ds(p, chan, stride=4), :].astype(BF16)

    def factor(p):
        gate = dot(normed, weight(p))
        value = dot(normed, weight(p + 1))
        return (jax.nn.sigmoid(gate) * value * live).astype(BF16)

    right_buf[z, core] = factor(2).reshape(rows, cols, chan)
    pl.semaphore_wait(barrier, 2 * subs + groups - 1)

    chunk_rows = rows // CHUNKS
    half = planes // 2
    last = half - 1

    def piece(origin, part, chunk):
        return right_buf.at[origin, part, pl.ds(chunk * chunk_rows, chunk_rows)]

    def behind(step):
        return lax.rem(z + 2 * planes - (2 * core - 1) * (1 + step), planes)

    def first_copy(way, chunk):
        return pltpu.make_async_remote_copy(
            src_ref=piece(z, core, chunk),
            dst_ref=piece(z, core, chunk),
            send_sem=first_send.at[way, chunk],
            recv_sem=ring_recv.at[0, core, chunk],
            device_id={"row": upper if way else lower, "sub": way},
            device_id_type=MESH,
        )

    def ring_copy(step, part, chunk):
        return pltpu.make_async_remote_copy(
            src_ref=piece(behind(step), part, chunk),
            dst_ref=piece(behind(step), part, chunk),
            send_sem=ring_send.at[step, part, chunk],
            recv_sem=ring_recv.at[step + 1, part, chunk],
            device_id={"row": ahead},
            device_id_type=MESH,
        )

    def ring_wait(step, part, chunk):
        block = piece(behind(step), part, chunk)
        pltpu.make_async_remote_copy(
            src_ref=block,
            dst_ref=block,
            send_sem=ring_send.at[0, part, chunk],
            recv_sem=ring_recv.at[step, part, chunk],
            device_id={"row": ahead},
            device_id_type=MESH,
        ).wait_recv()

    def mate_copy(ref, k):
        return pltpu.make_async_remote_copy(
            src_ref=ref,
            dst_ref=ref,
            send_sem=mate_send.at[k],
            recv_sem=mate_recv.at[k],
            device_id={"sub": mate},
            device_id_type=MESH,
        )

    for chunk in range(CHUNKS):
        for way in range(2):
            first_copy(way, chunk).start()
    mate_copy(right_buf.at[z, core], 0).start()
    left = factor(0)
    left_here[core] = left.reshape(rows, cols, chan)
    mate_copy(left_here.at[core], 1).start()
    left_buf[core] = left.astype(F32).reshape(rows, cols, chan)
    weight_buf[...] = w_att_ref[...].astype(F32)

    side = 1 - core
    half_chunks = CHUNKS // 2

    def products(origin, first, chunk):
        for j in range(chunk_rows):
            total = jnp.zeros((rows, chan), F32)
            for part in range(subs):
                right = right_buf[origin, part, (first + chunk) * chunk_rows + j].astype(F32)
                total = total + jnp.sum(left_buf[part] * right[None], axis=1)
            row = (chunk * chunk_rows + j) * rows
            stage_buf[row : row + rows, :] = total

    def part_copy(origin, h):
        return pltpu.make_async_remote_copy(
            src_ref=part_buf.at[origin, h],
            dst_ref=sum_buf.at[x, lax.rem(origin, per_owner), h],
            send_sem=part_send.at[origin, h],
            recv_sem=part_recv.at[x, lax.rem(origin, per_owner), h],
            device_id=in_plane(origin // per_owner),
            device_id_type=MESH,
        )

    def to_owner(origin, h):
        mine = origin // per_owner == g

        @pl.when(jnp.logical_not(mine))
        def _():
            part_buf[origin, h] = stage_buf[...]
            part_copy(origin, h).start()

        @pl.when(mine)
        def _():
            sum_buf[x, lax.rem(origin, per_owner), h] = stage_buf[...]

    def takes(origin, h):
        gap = lax.rem(z + planes - origin, planes)
        shared = (gap == 0) | (gap == half)
        return (shared & (side == h)) | (jnp.logical_not(shared) & ((gap < half) == (core == 1)))

    mate_copy(right_buf.at[z, mate], 0).wait_recv()
    mate_copy(left_here.at[mate], 1).wait_recv()
    left_buf[mate] = left_here[mate].astype(F32)
    for chunk in range(half_chunks):
        products(z, side * half_chunks, chunk)
    to_owner(z, side)

    def ring_step(step, carry):
        origin = behind(step)
        for chunk in range(CHUNKS):
            wanted = (step + 1 < last) | (chunk // half_chunks == side)
            for part in range(subs):
                ring_wait(step, part, chunk)

                @pl.when(wanted)
                def _():
                    ring_copy(step, part, chunk).start()

            h = chunk // half_chunks
            products(origin, h * half_chunks, chunk % half_chunks)
            if chunk % half_chunks == half_chunks - 1:
                to_owner(origin, h)
        return carry

    lax.fori_loop(0, last, ring_step, 0)
    far = lax.rem(z + half, planes)
    for k in range(half_chunks):
        for part in range(subs):
            ring_wait(last, part, side * half_chunks + k)
        products(far, side * half_chunks, k)
    to_owner(far, side)
    pl.semaphore_signal(mate_done, inc=1, device_id={"sub": mate}, device_id_type=MESH)
    for d in range(1, groups):
        pl.semaphore_signal(
            plane_done, inc=1, device_id=in_plane(lax.rem(g + d, groups)), device_id_type=MESH
        )

    tri_gate = jax.nn.sigmoid(dot(normed_buf[...], w_gate_ref[...]))

    block = rows * rows
    for p in range(per_owner):
        origin = g * per_owner + p
        for h in range(2):
            for d in range(chips):
                chip = lax.rem(x + d, chips)

                @pl.when(jnp.logical_not(takes(origin, h)) if d == 0 else chip >= 0)
                def _():
                    pltpu.make_async_remote_copy(
                        src_ref=part_buf.at[0, h],
                        dst_ref=sum_buf.at[chip, p, h],
                        send_sem=part_send.at[0, h],
                        recv_sem=part_recv.at[chip, p, h],
                        device_id=in_plane(g),
                        device_id_type=MESH,
                    ).wait_recv()

            total = sum_buf[0, p, h]
            for chip in range(1, chips):
                total = total + sum_buf[chip, p, h]
            at = p * block + h * (block // 2)
            tmp_buf[at : at + block // 2, :] = total
    for i in range(rows):
        tri_buf[i * cols : (i + 1) * cols, :] = tmp_buf[pl.ds(i, cols, stride=rows), :]

    hidden = norm_last(tri_buf[...], gain2_ref[...]).astype(BF16)
    pair_mid = pair_ref[...].reshape(flat, chan) + tri_gate * dot(hidden, w_tri_ref[...])
    mid_buf[...] = pair_mid
    att = norm_last(pair_mid, gain3_ref[...]).astype(BF16)
    att_buf[g] = att.reshape(rows, cols, chan)

    w_bias = jnp.concatenate(
        [w_bias_ref[...].astype(F32), jnp.zeros((8 - heads, chan), F32)], axis=0
    ).astype(BF16)

    for j in range(rows):
        bias_rows[j * 8 : (j + 1) * 8, :] = dot_nt(w_bias, att[j * cols : (j + 1) * cols, :])
    packed_rows = bias_z.shape[1]
    half_rows = rows // 2
    stacked = bias_rows[...].astype(BF16)
    message = jnp.zeros((packed_rows, chan), F32)
    for q in range(2):
        pick = one_hot(
            packed_rows,
            rows * 8,
            lambda r, c: c == (q * half_rows + lax.rem(r, half_rows)) * 8 + r // half_rows,
        )
        spread = one_hot(cols, chan, lambda r, c: c == r + q * cols)
        message = message + dot(dot(pick, stacked).astype(BF16), spread)
    bias_z[z] = message.astype(BF16)

    hops = planes // STRIDE
    near = (1, planes - 1, 2, 0)

    def bz_copy(source, target, sem):
        return pltpu.make_async_remote_copy(
            src_ref=bias_z.at[source],
            dst_ref=bias_z.at[source],
            send_sem=sem,
            recv_sem=bz_recv.at[source],
            device_id={"row": target},
            device_id_type=MESH,
        )

    def bz_wait(source):
        bz_copy(source, z, bz_far.at[0]).wait_recv()

    def bz_far_copy(m):
        return bz_copy(z, lax.rem(z + STRIDE * m, planes), bz_far.at[m])

    def bz_near_copy(m, n):
        source = lax.rem(z + STRIDE * m, planes)
        return pltpu.make_async_remote_copy(
            src_ref=bias_z.at[source],
            dst_ref=bias_x.at[g, lax.rem(source, per_owner)],
            send_sem=bz_near.at[m, n],
            recv_sem=bx_recv.at[g, lax.rem(source, per_owner)],
            device_id={"row": lax.rem(z + near[n], planes), **in_plane(source // per_owner)},
            device_id_type=MESH,
        )

    def leaves(m, n):
        return (lax.rem(z + STRIDE * m, planes) // per_owner != g) if near[n] == 0 else g >= 0

    by_distance = sorted(range(1, hops), key=lambda m: min(m, hops - m))

    def pass_bias(m):
        for n in range(len(near)):

            @pl.when(leaves(m, n))
            def _():
                bz_near_copy(m, n).start()

        source = lax.rem(z + STRIDE * m, planes)

        @pl.when(source // per_owner == g)
        def _():
            bias_x[g, lax.rem(source, per_owner)] = bias_z[source]

    pl.semaphore_wait(mate_done, 1)
    for m in reversed(by_distance):
        bz_far_copy(m).start()

    def att_copy(source, target, sem):
        return pltpu.make_async_remote_copy(
            src_ref=att_buf.at[source],
            dst_ref=att_buf.at[source],
            send_sem=sem,
            recv_sem=att_recv.at[source],
            device_id=target,
            device_id_type=MESH,
        )

    def att_across(d):
        return att_copy(g, {"col": lax.rem(x + d, chips)}, att_send.at[d])

    def att_over(c):
        return att_copy(c, {"sub": mate}, att_pass.at[c // subs])

    for d in sorted(range(1, chips), key=lambda d: -min(d, chips - d)):
        att_across(d).start()
    att_over(g).start()

    def att_weight(p):
        return weight_buf[pl.ds(p, chan, stride=4), :].astype(BF16)

    scale = (chan // heads) ** (-0.5)
    query_buf[...] = (dot(att, att_weight(0)) * scale).astype(BF16)
    gate_buf[...] = jax.nn.sigmoid(dot(att, att_weight(3)))
    key_weight, value_weight = att_weight(1), att_weight(2)

    def key_value(c):
        here = pl.ds(pl.multiple_of(c * cols, cols), cols)
        normed_rows = att_buf[c].reshape(flat, chan)
        key_buf[:, here, :] = dot(normed_rows, key_weight).astype(BF16).reshape(rows, cols, chan)
        value_buf[:, here, :] = (
            dot(normed_rows, value_weight).astype(BF16).reshape(rows, cols, chan)
        )

    def att_wait(c):
        att_copy(c, {"sub": mate}, att_pass.at[0]).wait_recv()

    def ring_sent(step, carry):
        for chunk in range(CHUNKS):
            wanted = (step + 1 < last) | (chunk // half_chunks == side)

            @pl.when(wanted)
            def _():
                for part in range(subs):
                    ring_copy(step, part, chunk).wait_send()

        return carry

    def parts_sent(origin, carry):
        for h in range(2):

            @pl.when(takes(origin, h) & (origin // per_owner != g))
            def _():
                part_copy(origin, h).wait_send()

        return carry

    lax.fori_loop(0, last, ring_sent, 0)
    for chunk in range(CHUNKS):
        for way in range(2):
            first_copy(way, chunk).wait_send()
    mate_copy(right_buf.at[z, core], 0).wait_send()
    mate_copy(left_here.at[core], 1).wait_send()
    lax.fori_loop(0, planes, parts_sent, 0)

    pl.semaphore_wait(plane_done, groups - 1)
    pass_bias(0)

    late = lax.rem(z + half, planes) // per_owner

    def take_rows(c):
        @pl.when(c != g)
        def _():
            att_wait(c)

        @pl.when((c != g) & (lax.rem(c, subs) == core))
        def _():
            att_over(c).start()

        key_value(c)

    def take_chip(of):
        def body(d, carry):
            c = lax.rem(late // subs + d, chips) * subs + of

            @pl.when(c != late)
            def _():
                take_rows(c)

            return carry

        return body

    def take_bias(k, carry):
        m = lax.rem(g + k + 2 * hops - z // STRIDE - hops // 2, hops)

        @pl.when(m != 0)
        def _():
            bz_wait(lax.rem(z + STRIDE * m, planes))
            pass_bias(m)

        return carry

    lax.fori_loop(1, chips + 1, take_chip(core), 0)
    lax.fori_loop(1, chips + 1, take_chip(mate), 0)
    lax.fori_loop(1, hops, take_bias, 0)
    take_rows(late)

    lane_head = lax.broadcasted_iota(jnp.int32, (cols, chan), 1) // (chan // heads)

    def raw_scores(i, carry):
        query = query_buf[pl.ds(pl.multiple_of(i * cols, cols), cols), :]
        stack = jnp.concatenate(
            [jnp.where(lane_head == h, query, jnp.zeros_like(query)) for h in range(heads)], axis=0
        )
        score_buf[i] = dot_nt(stack, key_buf[i])
        return carry

    lax.fori_loop(0, rows, raw_scores, 0, unroll=2)
    take_bias(0, 0)

    for d in range(groups):
        c = lax.rem(g + d, groups)
        for p in range(per_owner):
            source = g * per_owner + p
            came = (lax.rem(source + planes - z, STRIDE) != 0) if d == 0 else c >= 0

            @pl.when(came)
            def _():
                pltpu.make_async_remote_copy(
                    src_ref=bias_z.at[0],
                    dst_ref=bias_x.at[c, p],
                    send_sem=bz_near.at[0, 0],
                    recv_sem=bx_recv.at[c, p],
                    device_id=in_plane(g),
                    device_id_type=MESH,
                ).wait_recv()

    sums = [jnp.zeros((per_owner * packed_rows, residues), F32) for _ in range(2)]
    for d in range(groups):
        c = lax.rem(g + d, groups)
        piece = bias_x[c].reshape(per_owner * packed_rows, chan)
        for q in range(2):
            spread = one_hot(
                chan, residues, lambda r, k: (k - c * cols == r - q * cols) & (r >= q * cols) & (r < (q + 1) * cols)
            )
            sums[q] = sums[q] + dot(piece, spread)
    bias = jnp.zeros((heads * cols, residues), F32)
    for q in range(2):
        def match(r, c):
            h, j = r // cols, lax.rem(r, cols)
            p, j = j // rows, lax.rem(j, rows)
            return (j // half_rows == q) & (
                c == p * packed_rows + h * half_rows + lax.rem(j, half_rows)
            )

        bias = bias + dot(
            one_hot(heads * cols, per_owner * packed_rows, match), sums[q].astype(BF16)
        )
    bias_buf[...] = bias + (residue_live - 1.0) * MASK_PENALTY

    def attend(i, carry):
        scores = score_buf[i] + bias_buf[...]
        raised = jnp.exp(scores - jnp.max(scores, axis=-1, keepdims=True))
        weights = (raised * (1.0 / jnp.sum(raised, axis=-1, keepdims=True))).astype(BF16)
        mixed = dot(weights, value_buf[i])
        attended = jnp.zeros((cols, chan), F32)
        for h in range(heads):
            attended = jnp.where(lane_head == h, mixed[h * cols : (h + 1) * cols, :], attended)
        here = pl.ds(pl.multiple_of(i * cols, cols), cols)
        gated_buf[here, :] = (attended * gate_buf[here, :]).astype(BF16)
        return carry

    lax.fori_loop(0, rows, attend, 0, unroll=2)
    out_ref[...] = (mid_buf[...] + dot(gated_buf[...], w_out_ref[...])).reshape(rows, cols, chan)

    for m in range(hops):
        if m:
            bz_far_copy(m).wait_send()
        for n in range(len(near)):

            @pl.when(leaves(m, n))
            def _():
                bz_near_copy(m, n).wait_send()

    for d in range(chips):
        if d:
            att_across(d).wait_send()
        att_over(d * subs + core).wait_send()


def solution(mesh):
    planes = mesh.shape["row"]
    subs = mesh.shape["sub"]
    chips = mesh.shape["col"]
    groups = chips * subs

    def body(
        pair,
        residue_mask,
        tri_norm_gain,
        tri_in_weight,
        tri_gate_weight,
        tri_out_norm_gain,
        tri_out_weight,
        att_norm_gain,
        att_proj_weight,
        att_bias_weight,
        att_out_weight,
    ):
        rows, cols, chan = pair.shape
        heads = att_bias_weight.shape[1]
        residues = residue_mask.shape[0]
        flat = rows * cols
        per_owner = planes // groups
        packed = heads * rows // 2
        vmem = pl.BlockSpec(memory_space=pltpu.VMEM)
        dma = pltpu.SemaphoreType.DMA
        operands = (
            pair,
            residue_mask,
            tri_norm_gain[None, :],
            tri_in_weight.reshape(-1, chan),
            tri_gate_weight,
            tri_out_norm_gain[None, :],
            tri_out_weight,
            att_norm_gain[None, :],
            att_proj_weight.reshape(-1, chan),
            att_bias_weight.T,
            att_out_weight,
        )
        return pl.pallas_call(
            functools.partial(kernel, planes, chips, subs, heads),
            out_shape=jax.ShapeDtypeStruct(pair.shape, F32),
            in_specs=[vmem] * len(operands),
            out_specs=vmem,
            scratch_shapes=[
                pltpu.VMEM((planes, subs, rows, cols, chan), BF16),
                pltpu.VMEM((subs, rows, cols, chan), BF16),
                pltpu.VMEM((subs, rows, cols, chan), F32),
                pltpu.VMEM((flat, chan), BF16),
                pltpu.VMEM((4 * chan, chan), F32),
                pltpu.VMEM((rows * rows // 2, chan), F32),
                pltpu.VMEM((planes, 2, rows * rows // 2, chan), F32),
                pltpu.VMEM((chips, per_owner, 2, rows * rows // 2, chan), F32),
                pltpu.VMEM((flat, chan), F32),
                pltpu.VMEM((flat, chan), F32),
                pltpu.VMEM((groups, rows, cols, chan), BF16),
                pltpu.VMEM((rows, residues, chan), BF16),
                pltpu.VMEM((rows, residues, chan), BF16),
                pltpu.VMEM((flat, chan), BF16),
                pltpu.VMEM((flat, chan), F32),
                pltpu.VMEM((rows, heads * cols, residues), F32),
                pltpu.VMEM((flat, chan), F32),
                pltpu.VMEM((rows * 8, cols), F32),
                pltpu.VMEM((planes, packed, chan), BF16),
                pltpu.VMEM((groups, per_owner, packed, chan), BF16),
                pltpu.VMEM((heads * cols, residues), F32),
                pltpu.VMEM((flat, chan), BF16),
                dma((planes // 2, subs, CHUNKS)),
                dma((planes // 2, subs, CHUNKS)),
                dma((2, CHUNKS)),
                dma((2,)),
                dma((2,)),
                pltpu.SemaphoreType.REGULAR,
                pltpu.SemaphoreType.REGULAR,
                dma((planes, 2)),
                dma((chips, per_owner, 2)),
                dma((chips,)),
                dma((chips,)),
                dma((groups,)),
                dma((planes // STRIDE,)),
                dma((planes // STRIDE, 4)),
                dma((planes,)),
                dma((groups, per_owner)),
            ],
            compiler_params=pltpu.CompilerParams(
                collective_id=0, has_side_effects=True, vmem_limit_bytes=56 * 1024 * 1024
            ),
            name="pair_update",
        )(*operands)

    placed = (P(("parts", "row"), ("col", "sub"), None), P("parts")) + (P(),) * 9
    return jax.shard_map(
        body,
        mesh=mesh,
        in_specs=placed,
        out_specs=P(("parts", "row"), ("col", "sub"), None),
        check_vma=False,
    )
```

```python
import functools

import jax
import jax.numpy as jnp
from jax import lax
from jax.experimental import pallas as pl
from jax.experimental.pallas import tpu as pltpu
from jax.sharding import PartitionSpec as P

MESH = pl.DeviceIdType.MESH
EPSILON = 1e-05
MASK_PENALTY = 1000000000.0
F32 = jnp.float32
BF16 = jnp.bfloat16
CHUNKS = 4
STRIDE = 4


def norm_last(values_in, gain):
    center = jnp.mean(values_in, axis=-1, keepdims=True)
    centered = values_in - center
    variance = jnp.mean(centered * centered, axis=-1, keepdims=True)
    return centered * lax.rsqrt(variance + EPSILON) * gain


def dot(a, b):
    return lax.dot_general(a, b, (((1,), (0,)), ((), ())), preferred_element_type=F32)


def dot_nt(a, b):
    return lax.dot_general(a, b, (((1,), (1,)), ((), ())), preferred_element_type=F32)


def one_hot(rows, cols, match):
    r = lax.broadcasted_iota(jnp.int32, (rows, cols), 0)
    c = lax.broadcasted_iota(jnp.int32, (rows, cols), 1)
    return jnp.where(match(r, c), 1.0, 0.0).astype(BF16)


def kernel(
    planes,
    chips,
    subs,
    heads,
    pair_ref,
    mask_ref,
    gain1_ref,
    w_in_ref,
    w_gate_ref,
    gain2_ref,
    w_tri_ref,
    gain3_ref,
    w_att_ref,
    w_bias_ref,
    w_out_ref,
    out_ref,
    right_buf,
    left_here,
    left_buf,
    normed_buf,
    weight_buf,
    stage_buf,
    part_buf,
    sum_buf,
    tmp_buf,
    tri_buf,
    att_buf,
    key_buf,
    value_buf,
    query_buf,
    gate_buf,
    score_buf,
    mid_buf,
    bias_rows,
    bias_z,
    bias_x,
    bias_buf,
    gated_buf,
    ring_send,
    ring_recv,
    first_send,
    mate_send,
    mate_recv,
    mate_done,
    plane_done,
    part_send,
    part_recv,
    att_send,
    att_pass,
    att_recv,
    bz_far,
    bz_near,
    bz_recv,
    bx_recv,
):
    rows, cols, chan = pair_ref.shape
    groups = chips * subs
    flat = rows * cols
    per_owner = planes // groups
    residues = groups * cols
    z = lax.axis_index("row")
    x = lax.axis_index("col")
    core = lax.axis_index("sub")
    g = x * subs + core
    mate = 1 - core
    ahead = lax.rem(z + planes + 2 * core - 1, planes)
    upper = lax.rem(z + 1, planes)
    lower = lax.rem(z + planes - 1, planes)

    def in_plane(c):
        return {"col": c // subs, "sub": lax.rem(c, subs)}

    barrier = pltpu.get_barrier_semaphore()
    for other in (upper, lower):
        for s in range(subs):
            pl.semaphore_signal(
                barrier, inc=1, device_id={"row": other, "sub": s}, device_id_type=MESH
            )
    for d in range(1, groups):
        pl.semaphore_signal(
            barrier, inc=1, device_id=in_plane(lax.rem(g + d, groups)), device_id_type=MESH
        )

    pair = pair_ref[...].reshape(flat, chan)
    normed = norm_last(pair, gain1_ref[...]).astype(BF16)
    normed_buf[...] = normed
    residue_live = mask_ref[...].reshape(1, residues).astype(F32)
    live_rows_of = jnp.broadcast_to(residue_live, (chan, residues)).astype(BF16)
    live_rows = dot_nt(one_hot(16, residues, lambda r, c: c == r + z * rows), live_rows_of)
    live_cols = dot_nt(one_hot(cols, residues, lambda r, c: c == r + g * cols), live_rows_of)
    live = jnp.concatenate([live_rows[i : i + 1] * live_cols for i in range(rows)], axis=0)
    weight_buf[...] = w_in_ref[...].astype(F32)

    def weight(p):
        return weight_buf[pl.ds(p, chan, stride=4), :].astype(BF16)

    def factor(p):
        gate = dot(normed, weight(p))
        value = dot(normed, weight(p + 1))
        return (jax.nn.sigmoid(gate) * value * live).astype(BF16)

    right_buf[z, core] = factor(2).reshape(rows, cols, chan)
    pl.semaphore_wait(barrier, 2 * subs + groups - 1)

    chunk_rows = rows // CHUNKS
    half = planes // 2
    last = half - 1

    def piece(origin, part, chunk):
        return right_buf.at[origin, part, pl.ds(chunk * chunk_rows, chunk_rows)]

    def behind(step):
        return lax.rem(z + 2 * planes - (2 * core - 1) * (1 + step), planes)

    def first_copy(way, chunk):
        return pltpu.make_async_remote_copy(
            src_ref=piece(z, core, chunk),
            dst_ref=piece(z, core, chunk),
            send_sem=first_send.at[way, chunk],
            recv_sem=ring_recv.at[0, core, chunk],
            device_id={"row": upper if way else lower, "sub": way},
            device_id_type=MESH,
        )

    def ring_copy(step, part, chunk):
        return pltpu.make_async_remote_copy(
            src_ref=piece(behind(step), part, chunk),
            dst_ref=piece(behind(step), part, chunk),
            send_sem=ring_send.at[step, part, chunk],
            recv_sem=ring_recv.at[step + 1, part, chunk],
            device_id={"row": ahead},
            device_id_type=MESH,
        )

    def ring_wait(step, part, chunk):
        block = piece(behind(step), part, chunk)
        pltpu.make_async_remote_copy(
            src_ref=block,
            dst_ref=block,
            send_sem=ring_send.at[0, part, chunk],
            recv_sem=ring_recv.at[step, part, chunk],
            device_id={"row": ahead},
            device_id_type=MESH,
        ).wait_recv()

    def mate_copy(ref, k):
        return pltpu.make_async_remote_copy(
            src_ref=ref,
            dst_ref=ref,
            send_sem=mate_send.at[k],
            recv_sem=mate_recv.at[k],
            device_id={"sub": mate},
            device_id_type=MESH,
        )

    for chunk in range(CHUNKS):
        for way in range(2):
            first_copy(way, chunk).start()
    mate_copy(right_buf.at[z, core], 0).start()
    left = factor(0)
    left_here[core] = left.reshape(rows, cols, chan)
    mate_copy(left_here.at[core], 1).start()
    left_buf[core] = left.astype(F32).reshape(rows, cols, chan)
    weight_buf[...] = w_att_ref[...].astype(F32)

    side = 1 - core
    half_chunks = CHUNKS // 2

    def products(origin, first, chunk):
        for j in range(chunk_rows):
            total = jnp.zeros((rows, chan), F32)
            for part in range(subs):
                right = right_buf[origin, part, (first + chunk) * chunk_rows + j].astype(F32)
                total = total + jnp.sum(left_buf[part] * right[None], axis=1)
            row = (chunk * chunk_rows + j) * rows
            stage_buf[row : row + rows, :] = total

    def part_copy(origin, h):
        return pltpu.make_async_remote_copy(
            src_ref=part_buf.at[origin, h],
            dst_ref=sum_buf.at[x, lax.rem(origin, per_owner), h],
            send_sem=part_send.at[origin, h],
            recv_sem=part_recv.at[x, lax.rem(origin, per_owner), h],
            device_id=in_plane(origin // per_owner),
            device_id_type=MESH,
        )

    def to_owner(origin, h):
        mine = origin // per_owner == g

        @pl.when(jnp.logical_not(mine))
        def _():
            part_buf[origin, h] = stage_buf[...]
            part_copy(origin, h).start()

        @pl.when(mine)
        def _():
            sum_buf[x, lax.rem(origin, per_owner), h] = stage_buf[...]

    def takes(origin, h):
        gap = lax.rem(z + planes - origin, planes)
        shared = (gap == 0) | (gap == half)
        return (shared & (side == h)) | (jnp.logical_not(shared) & ((gap < half) == (core == 1)))

    mate_copy(right_buf.at[z, mate], 0).wait_recv()
    mate_copy(left_here.at[mate], 1).wait_recv()
    left_buf[mate] = left_here[mate].astype(F32)
    for chunk in range(half_chunks):
        products(z, side * half_chunks, chunk)
    to_owner(z, side)

    def ring_step(step, carry):
        origin = behind(step)
        for chunk in range(CHUNKS):
            wanted = (step + 1 < last) | (chunk // half_chunks == side)
            for part in range(subs):
                ring_wait(step, part, chunk)

                @pl.when(wanted)
                def _():
                    ring_copy(step, part, chunk).start()

            h = chunk // half_chunks
            products(origin, h * half_chunks, chunk % half_chunks)
            if chunk % half_chunks == half_chunks - 1:
                to_owner(origin, h)
        return carry

    lax.fori_loop(0, last, ring_step, 0)
    far = lax.rem(z + half, planes)
    for k in range(half_chunks):
        for part in range(subs):
            ring_wait(last, part, side * half_chunks + k)
        products(far, side * half_chunks, k)
    to_owner(far, side)
    pl.semaphore_signal(mate_done, inc=1, device_id={"sub": mate}, device_id_type=MESH)
    for d in range(1, groups):
        pl.semaphore_signal(
            plane_done, inc=1, device_id=in_plane(lax.rem(g + d, groups)), device_id_type=MESH
        )

    tri_gate = jax.nn.sigmoid(dot(normed_buf[...], w_gate_ref[...]))

    block = rows * rows
    for p in range(per_owner):
        origin = g * per_owner + p
        for h in range(2):
            for d in range(chips):
                chip = lax.rem(x + d, chips)

                @pl.when(jnp.logical_not(takes(origin, h)) if d == 0 else chip >= 0)
                def _():
                    pltpu.make_async_remote_copy(
                        src_ref=part_buf.at[0, h],
                        dst_ref=sum_buf.at[chip, p, h],
                        send_sem=part_send.at[0, h],
                        recv_sem=part_recv.at[chip, p, h],
                        device_id=in_plane(g),
                        device_id_type=MESH,
                    ).wait_recv()

            total = sum_buf[0, p, h]
            for chip in range(1, chips):
                total = total + sum_buf[chip, p, h]
            at = p * block + h * (block // 2)
            tmp_buf[at : at + block // 2, :] = total
    for i in range(rows):
        tri_buf[i * cols : (i + 1) * cols, :] = tmp_buf[pl.ds(i, cols, stride=rows), :]

    hidden = norm_last(tri_buf[...], gain2_ref[...]).astype(BF16)
    pair_mid = pair_ref[...].reshape(flat, chan) + tri_gate * dot(hidden, w_tri_ref[...])
    mid_buf[...] = pair_mid
    att = norm_last(pair_mid, gain3_ref[...]).astype(BF16)
    att_buf[g] = att.reshape(rows, cols, chan)

    w_bias = jnp.concatenate(
        [w_bias_ref[...].astype(F32), jnp.zeros((8 - heads, chan), F32)], axis=0
    ).astype(BF16)

    for j in range(rows):
        bias_rows[j * 8 : (j + 1) * 8, :] = dot_nt(w_bias, att[j * cols : (j + 1) * cols, :])
    packed_rows = bias_z.shape[1]
    half_rows = rows // 2
    stacked = bias_rows[...].astype(BF16)
    message = jnp.zeros((packed_rows, chan), F32)
    for q in range(2):
        pick = one_hot(
            packed_rows,
            rows * 8,
            lambda r, c: c == (q * half_rows + lax.rem(r, half_rows)) * 8 + r // half_rows,
        )
        spread = one_hot(cols, chan, lambda r, c: c == r + q * cols)
        message = message + dot(dot(pick, stacked).astype(BF16), spread)
    bias_z[z] = message.astype(BF16)

    hops = planes // STRIDE
    near = (1, planes - 1, 2, 0)

    def bz_copy(source, target, sem):
        return pltpu.make_async_remote_copy(
            src_ref=bias_z.at[source],
            dst_ref=bias_z.at[source],
            send_sem=sem,
            recv_sem=bz_recv.at[source],
            device_id={"row": target},
            device_id_type=MESH,
        )

    def bz_wait(source):
        bz_copy(source, z, bz_far.at[0]).wait_recv()

    def bz_far_copy(m):
        return bz_copy(z, lax.rem(z + STRIDE * m, planes), bz_far.at[m])

    def bz_near_copy(m, n):
        source = lax.rem(z + STRIDE * m, planes)
        return pltpu.make_async_remote_copy(
            src_ref=bias_z.at[source],
            dst_ref=bias_x.at[g, lax.rem(source, per_owner)],
            send_sem=bz_near.at[m, n],
            recv_sem=bx_recv.at[g, lax.rem(source, per_owner)],
            device_id={"row": lax.rem(z + near[n], planes), **in_plane(source // per_owner)},
            device_id_type=MESH,
        )

    def leaves(m, n):
        return (lax.rem(z + STRIDE * m, planes) // per_owner != g) if near[n] == 0 else g >= 0

    by_distance = sorted(range(1, hops), key=lambda m: min(m, hops - m))

    def pass_bias(m):
        for n in range(len(near)):

            @pl.when(leaves(m, n))
            def _():
                bz_near_copy(m, n).start()

        source = lax.rem(z + STRIDE * m, planes)

        @pl.when(source // per_owner == g)
        def _():
            bias_x[g, lax.rem(source, per_owner)] = bias_z[source]

    pl.semaphore_wait(mate_done, 1)
    for m in reversed(by_distance):
        bz_far_copy(m).start()
    pl.semaphore_wait(plane_done, groups - 1)
    pass_bias(0)

    def att_copy(source, target, sem):
        return pltpu.make_async_remote_copy(
            src_ref=att_buf.at[source],
            dst_ref=att_buf.at[source],
            send_sem=sem,
            recv_sem=att_recv.at[source],
            device_id=target,
            device_id_type=MESH,
        )

    def att_across(d):
        return att_copy(g, {"col": lax.rem(x + d, chips)}, att_send.at[d])

    def att_over(c):
        return att_copy(c, {"sub": mate}, att_pass.at[c // subs])

    for d in sorted(range(1, chips), key=lambda d: -min(d, chips - d)):
        att_across(d).start()
    att_over(g).start()

    def att_weight(p):
        return weight_buf[pl.ds(p, chan, stride=4), :].astype(BF16)

    scale = (chan // heads) ** (-0.5)
    query_buf[...] = (dot(att, att_weight(0)) * scale).astype(BF16)
    gate_buf[...] = jax.nn.sigmoid(dot(att, att_weight(3)))
    key_weight, value_weight = att_weight(1), att_weight(2)

    def key_value(c):
        here = pl.ds(pl.multiple_of(c * cols, cols), cols)
        normed_rows = att_buf[c].reshape(flat, chan)
        key_buf[:, here, :] = dot(normed_rows, key_weight).astype(BF16).reshape(rows, cols, chan)
        value_buf[:, here, :] = (
            dot(normed_rows, value_weight).astype(BF16).reshape(rows, cols, chan)
        )

    def att_wait(c):
        att_copy(c, {"sub": mate}, att_pass.at[0]).wait_recv()

    def ring_sent(step, carry):
        for chunk in range(CHUNKS):
            wanted = (step + 1 < last) | (chunk // half_chunks == side)

            @pl.when(wanted)
            def _():
                for part in range(subs):
                    ring_copy(step, part, chunk).wait_send()

        return carry

    def parts_sent(origin, carry):
        for h in range(2):

            @pl.when(takes(origin, h) & (origin // per_owner != g))
            def _():
                part_copy(origin, h).wait_send()

        return carry

    lax.fori_loop(0, last, ring_sent, 0)
    for chunk in range(CHUNKS):
        for way in range(2):
            first_copy(way, chunk).wait_send()
    mate_copy(right_buf.at[z, core], 0).wait_send()
    mate_copy(left_here.at[core], 1).wait_send()
    lax.fori_loop(0, planes, parts_sent, 0)

    late = lax.rem(z + half, planes) // per_owner

    def take_rows(c):
        @pl.when(c != g)
        def _():
            att_wait(c)

        @pl.when((c != g) & (lax.rem(c, subs) == core))
        def _():
            att_over(c).start()

        key_value(c)

    def take_chip(of):
        def body(d, carry):
            c = lax.rem(late // subs + d, chips) * subs + of

            @pl.when(c != late)
            def _():
                take_rows(c)

            return carry

        return body

    def take_bias(k, carry):
        m = lax.rem(g + k + 2 * hops - z // STRIDE - hops // 2, hops)

        @pl.when(m != 0)
        def _():
            bz_wait(lax.rem(z + STRIDE * m, planes))
            pass_bias(m)

        return carry

    lax.fori_loop(1, chips + 1, take_chip(core), 0)
    lax.fori_loop(1, chips + 1, take_chip(mate), 0)
    lax.fori_loop(1, hops, take_bias, 0)
    take_rows(late)

    lane_head = lax.broadcasted_iota(jnp.int32, (cols, chan), 1) // (chan // heads)

    def raw_scores(i, carry):
        query = query_buf[pl.ds(pl.multiple_of(i * cols, cols), cols), :]
        stack = jnp.concatenate(
            [jnp.where(lane_head == h, query, jnp.zeros_like(query)) for h in range(heads)], axis=0
        )
        score_buf[i] = dot_nt(stack, key_buf[i])
        return carry

    lax.fori_loop(0, rows, raw_scores, 0, unroll=4)
    take_bias(0, 0)

    for d in range(groups):
        c = lax.rem(g + d, groups)
        for p in range(per_owner):
            source = g * per_owner + p
            came = (lax.rem(source + planes - z, STRIDE) != 0) if d == 0 else c >= 0

            @pl.when(came)
            def _():
                pltpu.make_async_remote_copy(
                    src_ref=bias_z.at[0],
                    dst_ref=bias_x.at[c, p],
                    send_sem=bz_near.at[0, 0],
                    recv_sem=bx_recv.at[c, p],
                    device_id=in_plane(g),
                    device_id_type=MESH,
                ).wait_recv()

    sums = [jnp.zeros((per_owner * packed_rows, residues), F32) for _ in range(2)]
    for d in range(groups):
        c = lax.rem(g + d, groups)
        piece = bias_x[c].reshape(per_owner * packed_rows, chan)
        for q in range(2):
            spread = one_hot(
                chan, residues, lambda r, k: (k - c * cols == r - q * cols) & (r >= q * cols) & (r < (q + 1) * cols)
            )
            sums[q] = sums[q] + dot(piece, spread)
    bias = jnp.zeros((heads * cols, residues), F32)
    for q in range(2):
        def match(r, c):
            h, j = r // cols, lax.rem(r, cols)
            p, j = j // rows, lax.rem(j, rows)
            return (j // half_rows == q) & (
                c == p * packed_rows + h * half_rows + lax.rem(j, half_rows)
            )

        bias = bias + dot(
            one_hot(heads * cols, per_owner * packed_rows, match), sums[q].astype(BF16)
        )
    bias_buf[...] = bias + (residue_live - 1.0) * MASK_PENALTY

    def attend(i, carry):
        scores = score_buf[i] + bias_buf[...]
        raised = jnp.exp(scores - jnp.max(scores, axis=-1, keepdims=True))
        weights = (raised * (1.0 / jnp.sum(raised, axis=-1, keepdims=True))).astype(BF16)
        mixed = dot(weights, value_buf[i])
        attended = jnp.zeros((cols, chan), F32)
        for h in range(heads):
            attended = jnp.where(lane_head == h, mixed[h * cols : (h + 1) * cols, :], attended)
        here = pl.ds(pl.multiple_of(i * cols, cols), cols)
        gated_buf[here, :] = (attended * gate_buf[here, :]).astype(BF16)
        return carry

    lax.fori_loop(0, rows, attend, 0, unroll=4)
    out_ref[...] = (mid_buf[...] + dot(gated_buf[...], w_out_ref[...])).reshape(rows, cols, chan)

    for m in range(hops):
        if m:
            bz_far_copy(m).wait_send()
        for n in range(len(near)):

            @pl.when(leaves(m, n))
            def _():
                bz_near_copy(m, n).wait_send()

    for d in range(chips):
        if d:
            att_across(d).wait_send()
        att_over(d * subs + core).wait_send()


def solution(mesh):
    planes = mesh.shape["row"]
    subs = mesh.shape["sub"]
    chips = mesh.shape["col"]
    groups = chips * subs

    def body(
        pair,
        residue_mask,
        tri_norm_gain,
        tri_in_weight,
        tri_gate_weight,
        tri_out_norm_gain,
        tri_out_weight,
        att_norm_gain,
        att_proj_weight,
        att_bias_weight,
        att_out_weight,
    ):
        rows, cols, chan = pair.shape
        heads = att_bias_weight.shape[1]
        residues = residue_mask.shape[0]
        flat = rows * cols
        per_owner = planes // groups
        packed = heads * rows // 2
        vmem = pl.BlockSpec(memory_space=pltpu.VMEM)
        dma = pltpu.SemaphoreType.DMA
        operands = (
            pair,
            residue_mask,
            tri_norm_gain[None, :],
            tri_in_weight.reshape(-1, chan),
            tri_gate_weight,
            tri_out_norm_gain[None, :],
            tri_out_weight,
            att_norm_gain[None, :],
            att_proj_weight.reshape(-1, chan),
            att_bias_weight.T,
            att_out_weight,
        )
        return pl.pallas_call(
            functools.partial(kernel, planes, chips, subs, heads),
            out_shape=jax.ShapeDtypeStruct(pair.shape, F32),
            in_specs=[vmem] * len(operands),
            out_specs=vmem,
            scratch_shapes=[
                pltpu.VMEM((planes, subs, rows, cols, chan), BF16),
                pltpu.VMEM((subs, rows, cols, chan), BF16),
                pltpu.VMEM((subs, rows, cols, chan), F32),
                pltpu.VMEM((flat, chan), BF16),
                pltpu.VMEM((4 * chan, chan), F32),
                pltpu.VMEM((rows * rows // 2, chan), F32),
                pltpu.VMEM((planes, 2, rows * rows // 2, chan), F32),
                pltpu.VMEM((chips, per_owner, 2, rows * rows // 2, chan), F32),
                pltpu.VMEM((flat, chan), F32),
                pltpu.VMEM((flat, chan), F32),
                pltpu.VMEM((groups, rows, cols, chan), BF16),
                pltpu.VMEM((rows, residues, chan), BF16),
                pltpu.VMEM((rows, residues, chan), BF16),
                pltpu.VMEM((flat, chan), BF16),
                pltpu.VMEM((flat, chan), F32),
                pltpu.VMEM((rows, heads * cols, residues), F32),
                pltpu.VMEM((flat, chan), F32),
                pltpu.VMEM((rows * 8, cols), F32),
                pltpu.VMEM((planes, packed, chan), BF16),
                pltpu.VMEM((groups, per_owner, packed, chan), BF16),
                pltpu.VMEM((heads * cols, residues), F32),
                pltpu.VMEM((flat, chan), BF16),
                dma((planes // 2, subs, CHUNKS)),
                dma((planes // 2, subs, CHUNKS)),
                dma((2, CHUNKS)),
                dma((2,)),
                dma((2,)),
                pltpu.SemaphoreType.REGULAR,
                pltpu.SemaphoreType.REGULAR,
                dma((planes, 2)),
                dma((chips, per_owner, 2)),
                dma((chips,)),
                dma((chips,)),
                dma((groups,)),
                dma((planes // STRIDE,)),
                dma((planes // STRIDE, 4)),
                dma((planes,)),
                dma((groups, per_owner)),
            ],
            compiler_params=pltpu.CompilerParams(
                collective_id=0, has_side_effects=True, vmem_limit_bytes=56 * 1024 * 1024
            ),
            name="pair_update",
        )(*operands)

    placed = (P(("parts", "row"), ("col", "sub"), None), P("parts")) + (P(),) * 9
    return jax.shard_map(
        body,
        mesh=mesh,
        in_specs=placed,
        out_specs=P(("parts", "row"), ("col", "sub"), None),
        check_vma=False,
    )
```
